128 devices in a mesh: lat: 8 (over y, core), lon: 16 (over z, x).
Axes of the slice: x: 4, y: 4, z: 4, core: 2. Of those that a mesh axis runs over, the one named last changes fastest.
Arguments:
- grid_in: bfloat16 [262144, 227], P(('lat', 'lon')), may hold values from -6 to 6
- mesh_emb: bfloat16 [65536, 512], P(('lat', 'lon')), may hold values from -6 to 6
- enc_dest: int32 [262144, 2], P(('lat', 'lon')), may hold values from 0 to 127, as said below
- enc_node: int32 [262144, 2], P(('lat', 'lon')), may hold values from 0 to 511
- enc_dist: float32 [262144, 2], P(('lat', 'lon')), may hold values from 0.2 to 2
- dec_dist: float32 [262144, 2], P(('lat', 'lon')), may hold values from 0.2 to 2
- mesh_src: int32 [65536, 8], P(('lat', 'lon')), may hold values from 0 to 65535, as said below
- proc_dist: float32 [65536, 8], P(('lat', 'lon')), may hold values from 0.2 to 2
- w_grid_in: bfloat16 [227, 512], replicated, may hold values from -0.375 to 0.375
- w_enc_src: bfloat16 [512, 512], replicated, may hold values from -0.25 to 0.25
- w_enc_dist: float32 [512], replicated, may hold values from -6 to 6
- w_mesh_self: bfloat16 [512, 512], replicated, may hold values from -0.25 to 0.25
- w_mesh_agg: bfloat16 [512, 512], replicated, may hold values from -0.09375 to 0.09375
- w_proc_send: bfloat16 [512, 512], replicated, may hold values from -0.25 to 0.25
- w_proc_recv: bfloat16 [512, 512], replicated, may hold values from -0.25 to 0.25
- w_proc_dist: float32 [512], replicated, may hold values from -6 to 6
- w_proc_self: bfloat16 [512, 512], replicated, may hold values from -0.25 to 0.25
- w_proc_agg: bfloat16 [512, 512], replicated, may hold values from -0.125 to 0.125
- w_dec_send: bfloat16 [512, 512], replicated, may hold values from -0.25 to 0.25
- w_dec_recv: bfloat16 [512, 512], replicated, may hold values from -0.25 to 0.25
- w_dec_dist: float32 [512], replicated, may hold values from -6 to 6
- w_grid_self: bfloat16 [512, 512], replicated, may hold values from -0.25 to 0.25
- w_grid_agg: bfloat16 [512, 512], replicated, may hold values from -0.1875 to 0.1875
- w_grid_out: bfloat16 [512, 227], replicated, may hold values from -0.25 to 0.25
Outputs:
- pred: bfloat16 [262144, 227], P(('lat', 'lon'))
The draws below stay inside these ranges and needn't reach their ends.
Inputs may be any that keep to these rules, and one draw needn't show every extreme that they name: `enc_dest`: patch p lies at patch row p // 16 and column p % 16; cell c lies on the device of index c // 2048 (lat index times 16 plus lon index). The first entry of a row is the cell's own patch. The second is a different patch whose row differs by at most one (no wrap) and whose column differs by at most one, columns wrapping around. Among the cells of one device, no patch is named in the second entry by more than 512 cells, and some patch by exactly 512. `mesh_src`: node n lies in patch n // 512. Every sender lies in the receiver's patch or in one whose row differs by at most one (no wrap) and whose column differs by at most one, columns wrapping around.
All inputs are finite; a program needn't handle non-finite values.
Results may differ from the reference program's by a relative error of at most 0.014.
Values may be sent and summed in bfloat16 or wider, within the bound.
A program may use at most 128 MiB of HBM per device.

```python
import math
import jax
import jax.numpy as jnp

LATENT = 512
VARS = 227
GRID_DEV = 2048
MESH_DEV = 512
DEG = 8
GRID = 262144
MESH = 65536
CAP = 512
N_LAT = 8
N_LON = 16
DEVICES = 128


def draw_mesh_src(key, part):
    first, second, third = jax.random.split(key, 3)
    index = jnp.arange(MESH, dtype=jnp.int32)
    patch = index // MESH_DEV
    row = patch // N_LON
    column = patch % N_LON
    shift_row = jax.random.randint(first, (MESH, DEG), -1, 2, dtype=jnp.int32)
    shift_col = jax.random.randint(second, (MESH, DEG), -1, 2, dtype=jnp.int32)
    node = jax.random.randint(third, (MESH, DEG), 0, MESH_DEV, dtype=jnp.int32)
    new_row = jnp.clip(row[:, None] + shift_row, 0, N_LAT - 1)
    new_col = (column[:, None] + shift_col) % N_LON
    return ((new_row * N_LON + new_col) * MESH_DEV + node).astype(jnp.int32)


def draw_enc_dest(key, part):
    first, second = jax.random.split(jax.random.fold_in(key, 71), 2)
    device = jnp.arange(DEVICES, dtype=jnp.int32)
    row = device // N_LON
    column = device % N_LON
    step_rows = jnp.array([-1, -1, -1, 0, 0, 1, 1, 1], dtype=jnp.int32)
    step_cols = jnp.array([-1, 0, 1, -1, 1, -1, 0, 1], dtype=jnp.int32)
    moved = row[:, None] + step_rows[None, :]
    valid = (moved >= 0) & (moved < N_LAT)
    score = jnp.where(valid, 0, 8).astype(jnp.int32) + jnp.arange(8, dtype=jnp.int32)[None, :]
    order = jnp.argsort(score, axis=1).astype(jnp.int32)
    count = jnp.sum(valid.astype(jnp.int32), axis=1)
    busy = jax.random.randint(first, (DEVICES,), 0, count, dtype=jnp.int32)
    keys = jax.random.split(second, DEVICES)
    perms = jax.vmap(lambda k: jax.random.permutation(k, GRID_DEV))(keys).astype(jnp.int32)
    ranks = jnp.argsort(perms, axis=1).astype(jnp.int32)
    others = (busy[:, None] + 1 + (ranks - CAP) % (count[:, None] - 1)) % count[:, None]
    pick = jnp.where(ranks < CAP, busy[:, None], others).astype(jnp.int32)
    direction = jnp.take_along_axis(order, pick, axis=1)
    new_row = row[:, None] + step_rows[direction]
    new_col = (column[:, None] + step_cols[direction]) % N_LON
    second_patch = (new_row * N_LON + new_col).astype(jnp.int32)
    first_patch = jnp.broadcast_to(device[:, None], (DEVICES, GRID_DEV)).astype(jnp.int32)
    both = jnp.stack([first_patch, second_patch], axis=-1)
    return both.reshape(GRID, 2).astype(jnp.int32)


def place_ends(values, rng, least, top_value):
    dims = values.shape
    spot = [jax.random.randint(jax.random.fold_in(rng, axis), (), 0, dims[axis]) for axis in range(len(dims))]
    values = values.at[tuple(spot)].set(least)
    longest = dims.index(max(dims))
    spot[longest] = (spot[longest] + 1) % dims[longest]
    return values.at[tuple(spot)].set(top_value)


def level_of(key, extent, cuts, least, top_value):
    factor_of = 1.0
    for dim, parts in cuts:
        heights = jax.random.uniform(jax.random.fold_in(jax.random.fold_in(key, 6), dim), (parts,), jnp.float32, least / len(cuts), top_value / len(cuts))
        factor_of = factor_of * jnp.repeat(jnp.exp(heights), extent[dim] // parts).reshape((-1,) + (1,) * (len(extent) - 1 - dim))
    return factor_of


def centred(key, dims, width, bound, shards=(), kind=jnp.bfloat16):
    result = width * jax.random.normal(key, dims, jnp.float32)
    if shards:
        result = result * level_of(key, dims, shards, -0.22, 0.18)
    return jnp.clip(result, -bound, bound).astype(kind)


def setup_inputs(seed: int = 0) -> dict:
    seeds = jax.random.split(jax.random.key(seed), 25)
    grid_in = centred(seeds[0], (GRID, VARS), 1.0, 6.0, ((0, 128),))
    mesh_emb = centred(seeds[1], (MESH, LATENT), 1.0, 6.0, ((0, 128),))
    enc_dest = draw_enc_dest(jax.random.fold_in(seeds[24], 71), 0)
    enc_node = place_ends(jax.random.randint(seeds[3], (GRID, 2), 0, MESH_DEV), jax.random.fold_in(seeds[3], 1), 0, MESH_DEV - 1).astype(jnp.int32)
    enc_dist = jnp.clip(jnp.exp(math.log(2.0) - 2.3025851 * jax.random.uniform(seeds[4], (GRID, 2), jnp.float32) ** level_of(seeds[4], (GRID, 2), ((0, 128),), -0.2, 0.2)), 0.2, 2.0)
    dec_dist = jnp.clip(jnp.exp(math.log(2.0) - 2.3025851 * jax.random.uniform(seeds[5], (GRID, 2), jnp.float32) ** level_of(seeds[5], (GRID, 2), ((0, 128),), -0.2, 0.2)), 0.2, 2.0)
    mesh_src = draw_mesh_src(jax.random.fold_in(seeds[24], 71), 0)
    proc_dist = jnp.clip(jnp.exp(math.log(2.0) - 2.3025851 * jax.random.uniform(seeds[7], (MESH, DEG), jnp.float32) ** level_of(seeds[7], (MESH, DEG), ((0, 128),), -0.2, 0.2)), 0.2, 2.0)
    w_grid_in = centred(seeds[8], (VARS, LATENT), VARS ** -0.5, 0.375)
    w_enc_src = centred(seeds[9], (LATENT, LATENT), LATENT ** -0.5, 0.25)
    w_enc_dist = centred(seeds[10], (LATENT,), 1.0, 6.0, (), jnp.float32)
    w_mesh_self = centred(seeds[11], (LATENT, LATENT), LATENT ** -0.5, 0.25)
    w_mesh_agg = centred(seeds[12], (LATENT, LATENT), (8 * LATENT) ** -0.5, 0.09375)
    w_proc_send = centred(seeds[13], (LATENT, LATENT), LATENT ** -0.5, 0.25)
    w_proc_recv = centred(seeds[14], (LATENT, LATENT), LATENT ** -0.5, 0.25)
    w_proc_dist = centred(seeds[15], (LATENT,), 1.0, 6.0, (), jnp.float32)
    w_proc_self = centred(seeds[16], (LATENT, LATENT), LATENT ** -0.5, 0.25)
    w_proc_agg = centred(seeds[17], (LATENT, LATENT), (4 * LATENT) ** -0.5, 0.125)
    w_dec_send = centred(seeds[18], (LATENT, LATENT), LATENT ** -0.5, 0.25)
    w_dec_recv = centred(seeds[19], (LATENT, LATENT), LATENT ** -0.5, 0.25)
    w_dec_dist = centred(seeds[20], (LATENT,), 1.0, 6.0, (), jnp.float32)
    w_grid_self = centred(seeds[21], (LATENT, LATENT), LATENT ** -0.5, 0.25)
    w_grid_agg = centred(seeds[22], (LATENT, LATENT), (2 * LATENT) ** -0.5, 0.1875)
    w_grid_out = centred(seeds[23], (LATENT, VARS), LATENT ** -0.5, 0.25)
    return dict(grid_in=grid_in, mesh_emb=mesh_emb, enc_dest=enc_dest, enc_node=enc_node, enc_dist=enc_dist, dec_dist=dec_dist, mesh_src=mesh_src, proc_dist=proc_dist, w_grid_in=w_grid_in, w_enc_src=w_enc_src, w_enc_dist=w_enc_dist, w_mesh_self=w_mesh_self, w_mesh_agg=w_mesh_agg, w_proc_send=w_proc_send, w_proc_recv=w_proc_recv, w_proc_dist=w_proc_dist, w_proc_self=w_proc_self, w_proc_agg=w_proc_agg, w_dec_send=w_dec_send, w_dec_recv=w_dec_recv, w_dec_dist=w_dec_dist, w_grid_self=w_grid_self, w_grid_agg=w_grid_agg, w_grid_out=w_grid_out)


def reference(grid_in, mesh_emb, enc_dest, enc_node, enc_dist, dec_dist, mesh_src, proc_dist, w_grid_in, w_enc_src, w_enc_dist, w_mesh_self, w_mesh_agg, w_proc_send, w_proc_recv, w_proc_dist, w_proc_self, w_proc_agg, w_dec_send, w_dec_recv, w_dec_dist, w_grid_self, w_grid_agg, w_grid_out):
    grid_h = jax.nn.silu(jnp.dot(grid_in, w_grid_in, preferred_element_type=jnp.float32)).astype(jnp.bfloat16)
    enc_proj = jnp.dot(grid_h, w_enc_src, preferred_element_type=jnp.float32)
    enc_msg = jax.nn.silu(enc_proj[:, None, :] + enc_dist[:, :, None] * w_enc_dist).astype(jnp.bfloat16)
    target = (enc_dest * MESH_DEV + enc_node).astype(jnp.int32).reshape(-1)
    enc_agg = jax.ops.segment_sum(enc_msg.reshape(-1, LATENT).astype(jnp.float32), target, num_segments=MESH).astype(jnp.bfloat16)
    mesh_upd = jnp.dot(mesh_emb, w_mesh_self, preferred_element_type=jnp.float32) + jnp.dot(enc_agg, w_mesh_agg, preferred_element_type=jnp.float32)
    mesh_h = (mesh_emb.astype(jnp.float32) + jax.nn.silu(mesh_upd)).astype(jnp.bfloat16)
    proc_send = jnp.dot(mesh_h, w_proc_send, preferred_element_type=jnp.float32).astype(jnp.bfloat16)
    proc_recv = jnp.dot(mesh_h, w_proc_recv, preferred_element_type=jnp.float32)
    gathered = jnp.take(proc_send, mesh_src.reshape(-1), axis=0).reshape(MESH, DEG, LATENT).astype(jnp.float32)
    proc_msg = jax.nn.silu(gathered + proc_recv[:, None, :] + proc_dist[:, :, None] * w_proc_dist)
    proc_agg = jnp.sum(proc_msg, axis=1).astype(jnp.bfloat16)
    proc_upd = jnp.dot(mesh_h, w_proc_self, preferred_element_type=jnp.float32) + jnp.dot(proc_agg, w_proc_agg, preferred_element_type=jnp.float32)
    mesh_out = (mesh_h.astype(jnp.float32) + jax.nn.silu(proc_upd)).astype(jnp.bfloat16)
    dec_send = jnp.dot(mesh_out, w_dec_send, preferred_element_type=jnp.float32).astype(jnp.bfloat16)
    dec_recv = jnp.dot(grid_h, w_dec_recv, preferred_element_type=jnp.float32)
    fetched = jnp.take(dec_send, target, axis=0).reshape(GRID, 2, LATENT).astype(jnp.float32)
    dec_msg = jax.nn.silu(fetched + dec_recv[:, None, :] + dec_dist[:, :, None] * w_dec_dist)
    dec_agg = jnp.sum(dec_msg, axis=1).astype(jnp.bfloat16)
    grid_upd = jnp.dot(grid_h, w_grid_self, preferred_element_type=jnp.float32) + jnp.dot(dec_agg, w_grid_agg, preferred_element_type=jnp.float32)
    grid_z = jax.nn.silu(grid_upd).astype(jnp.bfloat16)
    pred = grid_in.astype(jnp.float32) + jnp.dot(grid_z, w_grid_out, preferred_element_type=jnp.float32)
    return pred.astype(jnp.bfloat16)
```

```python
import functools

import jax
import jax.numpy as jnp
from jax import lax
from jax.experimental import pallas as pl
from jax.experimental.pallas import tpu as pltpu
from jax.sharding import PartitionSpec as P

BF16 = jnp.bfloat16
F32 = jnp.float32
I32 = jnp.int32
QUARTERS = 4

PARTNER, CROSS, LEFT, RIGHT = range(4)

XL, XR, PL_, PR, OL, OR, XC, PC = range(8)

U_OWN, U_PART, U_CROSS = 0, 1, 3
U_SIDE = {"own": (2, 5), "part": (4, 7), "cross": (6, 8)}
UNITS = 9

ENC_SEMS = 2 * QUARTERS + 2 + 2 * QUARTERS + 2
HALO_SEMS = 8 * QUARTERS


def silu(v):
    h = 0.5 * v
    return h + h * jnp.tanh(h)


def mm(a, b):
    return jnp.dot(a, b, preferred_element_type=F32)


def one_hot(keys, base, width):
    lane = lax.broadcasted_iota(I32, keys.shape, 1)
    shifted = keys - base
    pieces = [
        jnp.where(shifted == lane + g * 128, 1.0, 0.0).astype(BF16) for g in range(width // 128)
    ]
    return jnp.concatenate(pieces, axis=1)


def kernel(
    n_lat,
    n_lon,
    weights,
    grid_t,
    emb,
    dest,
    node,
    enc_d,
    dec_d,
    src,
    proc_d,
    w_enc_dist,
    w_proc_dist,
    w_dec_dist,
    *refs,
):
    hbm = dict(zip(weights, refs[: len(weights)]))
    (
        out,
        wv_all,
        w_in,
        w_out,
        cell_keys,
        cell_rows,
        cell_cols,
        key1_lanes,
        key0_lanes,
        proc_lanes,
        proc_cols,
        grid_h,
        msg,
        sb,
        rb,
        ss,
        own_c,
        pre,
        mesh_h,
        table1,
        table2,
        acc,
        u_buf,
        w_sems,
        enc_send,
        enc_recv,
        h1_send,
        h1_recv,
        h2_send,
        h2_recv,
    ) = refs[len(weights) :]
    m, width = emb.shape
    cells = grid_t.shape[1]
    degree = src.shape[0]
    quarter = m // QUARTERS
    half = m // 2
    block = min(256, cells)
    wide = min(512, cells)

    lat = lax.axis_index("lat")
    lon = lax.axis_index("lon")
    core = lat % 2
    toward = 1 - 2 * core
    partner = (lat + toward, lon)
    cross = ((lat - toward + n_lat) % n_lat, lon)
    left = (lat, (lon - 1 + n_lon) % n_lon)
    right = (lat, (lon + 1) % n_lon)
    peers = (partner, cross, left, right)

    square = [name for name in weights if name not in ("w_grid_in", "w_grid_out")]
    w_at = {name: wv_all.at[i] for i, name in enumerate(square)}
    w_at["w_grid_in"] = w_in
    w_at["w_grid_out"] = w_out
    fetches = {
        name: pltpu.make_async_copy(hbm[name], w_at[name], w_sems.at[i])
        for i, name in enumerate(weights)
    }
    for name in weights:
        fetches[name].start()
    barrier = pltpu.get_barrier_semaphore()
    for peer in peers:
        pl.semaphore_signal(
            barrier, inc=1, device_id=peer, device_id_type=pl.DeviceIdType.MESH
        )

    def weight(name):
        return w_at[name][...]

    def remote(src_ref, dst_ref, send, recv, i, peer):
        return pltpu.make_async_remote_copy(
            src_ref=src_ref,
            dst_ref=dst_ref,
            send_sem=send.at[i],
            recv_sem=recv.at[i],
            device_id=peers[peer],
            device_id_type=pl.DeviceIdType.MESH,
        )

    shift = m.bit_length() - 1
    lon_shift = n_lon.bit_length() - 1

    def places(patch):
        d_row = (patch >> lon_shift) - lat
        side = ((patch & (n_lon - 1)) - lon + 1) & (n_lon - 1)
        return d_row == 0, d_row == toward, side

    def gather_key(patch, at):
        own, part, side = places(patch)
        upper = (at >= half).astype(I32)
        centre = jnp.where(own, U_OWN, jnp.where(part, U_PART, U_CROSS)) * m + at
        first = jnp.where(own, U_SIDE["own"][0], jnp.where(part, U_SIDE["part"][0], U_SIDE["cross"][0]))
        second = jnp.where(own, U_SIDE["own"][1], jnp.where(part, U_SIDE["part"][1], U_SIDE["cross"][1]))
        unit = jnp.where(upper == 1, second, first)
        beside = unit * m + jnp.where(side == 2, half, 0) + at - upper * half
        return jnp.where(side == 1, centre, beside)

    patch1 = dest[1:2, :]
    node1 = node[1:2, :]
    own1, part1, side1 = places(patch1)
    slot_l = jnp.where(own1, OL, jnp.where(part1, PL_, XL))
    slot_r = jnp.where(own1, OR, jnp.where(part1, PR, XR))
    slot_c = jnp.where(part1, PC, XC)
    slot = jnp.where(side1 == 0, slot_l, jnp.where(side1 == 2, slot_r, slot_c))
    cell_rows[0:1, :] = slot * m + node1
    cell_rows[1:2, :] = node[0:1, :]
    cell_keys[...] = jnp.zeros_like(cell_keys)
    cell_keys[0:1, :] = node[0:1, :].astype(F32)
    cell_keys[1:2, :] = gather_key(patch1, node1).astype(F32)
    cell_keys[2:4, :] = enc_d[...]
    cell_keys[4:6, :] = dec_d[...]
    cell_cols[...] = jnp.transpose(cell_keys[...])
    mesh_key = gather_key(src[...] >> shift, src[...] & (m - 1)).astype(F32)
    mesh_key_t = jnp.transpose(mesh_key)
    proc_cols[...] = jnp.transpose(proc_d[...])
    for j in range(degree):
        proc_lanes[j] = jnp.broadcast_to(mesh_key_t[:, j : j + 1], (m, 128)).astype(I32)

    fetches["w_grid_in"].wait()
    fetches["w_enc_src"].wait()

    def embed(b, carry):
        rows = pl.ds(pl.multiple_of(b * block, block), block)
        part = grid_t[:, rows]
        h = silu(
            lax.dot_general(part, w_in[...], (((0,), (0,)), ((), ())), preferred_element_type=F32)
        ).astype(BF16)
        grid_h[rows, :] = h
        e = mm(h, weight("w_enc_src"))
        cols = cell_cols[rows, :]
        for k in range(2):
            msg[k, rows, :] = silu(e + cols[:, 2 + k : 3 + k] * w_enc_dist[...]).astype(BF16)
        key0_lanes[rows, :] = jnp.broadcast_to(cols[:, 0:1], (block, 128)).astype(I32)
        key1_lanes[rows, :] = jnp.broadcast_to(cols[:, 1:2], (block, 128)).astype(I32)
        return carry

    lax.fori_loop(0, cells // block, embed, 0)
    pl.semaphore_wait(barrier, 4)

    def enc_x(side, q):
        rows = pl.ds(q * quarter, quarter)
        return remote(
            sb.at[side, rows], rb.at[side, rows], enc_send, enc_recv, 2 * q + side, CROSS
        )

    def enc_p(side):
        return remote(
            sb.at[2 + side], rb.at[2 + side], enc_send, enc_recv, 2 * QUARTERS + side, PARTNER
        )

    def enc_side(side, q):
        rows = pl.ds(q * quarter, quarter)
        return remote(
            ss.at[side, rows],
            rb.at[4 + side, rows],
            enc_send,
            enc_recv,
            2 * QUARTERS + 2 + 2 * q + side,
            LEFT if side == 0 else RIGHT,
        )

    def enc_c(which):
        return remote(
            sb.at[XC + which],
            rb.at[XC + which],
            enc_send,
            enc_recv,
            4 * QUARTERS + 2 + which,
            CROSS if which == 0 else PARTNER,
        )

    def relay_sums(q):
        rows = pl.ds(q * quarter, quarter)
        for side in range(2):
            enc_x(side, q).wait_recv()
            if q == 0:
                enc_p(side).wait_recv()
            total = (
                sb[4 + side, rows, :].astype(F32)
                + rb[side, rows, :].astype(F32)
                + rb[2 + side, rows, :].astype(F32)
            )
            ss[side, rows, :] = total.astype(BF16)
        for side in range(2):
            enc_side(side, q).start()

    def scatter(row, base, which):
        keys = cell_rows[row : row + 1, :] - base
        sel = jnp.where(lax.broadcasted_iota(I32, (m, cells), 0) == keys, 1.0, 0.0).astype(BF16)
        return mm(sel, msg[which])

    def partial_step(s, carry):
        sb[s] = scatter(0, s * m, 1).astype(BF16)

        @pl.when(s == XR)
        def _():
            for q in range(QUARTERS):
                for side in range(2):
                    enc_x(side, q).start()

        @pl.when(s == PR)
        def _():
            for side in range(2):
                enc_p(side).start()

        @pl.when(s == OR)
        def _():
            relay_sums(0)

        @pl.when(s == XC)
        def _():
            enc_c(0).start()
            relay_sums(1)

        @pl.when(s == PC)
        def _():
            enc_c(1).start()
            relay_sums(2)

        return carry

    lax.fori_loop(0, 8, partial_step, 0)
    own_c[...] = scatter(1, 0, 0)
    relay_sums(3)

    fetches["w_mesh_self"].wait()
    fetches["w_mesh_agg"].wait()
    fetches["w_proc_send"].wait()
    pre[...] = mm(emb[...], weight("w_mesh_self"))
    enc_c(0).wait_recv()
    enc_c(1).wait_recv()

    def halo(table, send, recv):
        def own(q, peer):
            src_ref = table.at[U_OWN, pl.ds(q * quarter, quarter)]
            if peer == PARTNER:
                dst = table.at[U_PART, pl.ds(q * quarter, quarter)]
            elif peer == CROSS:
                dst = table.at[U_CROSS, pl.ds(q * quarter, quarter)]
            else:
                dst = side_rows("own", 1 if peer == LEFT else 0, q)
            return remote(src_ref, dst, send, recv, 4 * q + peer, peer)

        def side_rows(owner, side, q):
            unit = U_SIDE[owner][q // 2]
            return table.at[unit, pl.ds(side * half + (q % 2) * quarter, quarter)]

        def forward(side, q, peer):
            dst = side_rows("part" if peer == PARTNER else "cross", side, q)
            index = 4 * QUARTERS + 4 * q + 2 * side + peer
            return remote(side_rows("own", side, q), dst, send, recv, index, peer)

        def start_own(q):
            for peer in (LEFT, RIGHT, CROSS, PARTNER):
                own(q, peer).start()

        def pass_on(q):
            own(q, RIGHT).wait_recv()
            own(q, LEFT).wait_recv()
            for side in range(2):
                forward(side, q, CROSS).start()
                forward(side, q, PARTNER).start()

        def wait_forwarded(peer, quarters):
            for q in quarters:
                for side in range(2):
                    forward(side, q, peer).wait_recv()

        def before(u):
            @pl.when(u == 1)
            def _():
                for q in range(QUARTERS):
                    own(q, PARTNER).wait_recv()

            @pl.when(u == 2)
            def _():
                pass_on(0)
                pass_on(1)

            @pl.when(u == 3)
            def _():
                for q in range(QUARTERS):
                    own(q, CROSS).wait_recv()

            @pl.when(u == 4)
            def _():
                pass_on(2)
                wait_forwarded(PARTNER, (0, 1))

            @pl.when(u == 5)
            def _():
                pass_on(3)

            @pl.when(u == 6)
            def _():
                wait_forwarded(CROSS, (0, 1))

            @pl.when(u == 7)
            def _():
                wait_forwarded(PARTNER, (2, 3))

        def before_last():
            wait_forwarded(CROSS, (2, 3))

        def finish():
            for q in range(QUARTERS):
                for peer in range(4):
                    own(q, peer).wait_send()
                for side in range(2):
                    for peer in (PARTNER, CROSS):
                        forward(side, q, peer).wait_send()

        return start_own, before, before_last, finish

    start1, before1, last1, finish1 = halo(table1, h1_send, h1_recv)
    start2, before2, last2, finish2 = halo(table2, h2_send, h2_recv)

    for q in range(QUARTERS):
        rows = pl.ds(q * quarter, quarter)
        for side in range(2):
            enc_side(side, q).wait_recv()
        total = own_c[rows, :]
        for i in range(4, 8):
            total = total + rb[i, rows, :].astype(F32)
        upd = pre[rows, :] + mm(total.astype(BF16), weight("w_mesh_agg"))
        h = (emb[rows, :].astype(F32) + silu(upd)).astype(BF16)
        mesh_h[rows, :] = h
        table1[U_OWN, rows, :] = mm(h, weight("w_proc_send")).astype(BF16)
        start1(q)

    fetches["w_proc_recv"].wait()
    fetches["w_proc_self"].wait()
    fetches["w_proc_agg"].wait()
    fetches["w_dec_send"].wait()
    pre[...] = mm(mesh_h[...], weight("w_proc_recv"))
    for j in range(degree):
        acc[pl.ds(j * m, m), :] = pre[...] + proc_cols[:, j : j + 1] * w_proc_dist[...]
    own_c[...] = mm(mesh_h[...], weight("w_proc_self"))

    def proc_rows(j):
        return pl.ds(pl.multiple_of(j * m, m), m)

    def proc_unit(u, carry):
        before1(u)

        def edge(j, c):
            rows = proc_rows(j)
            acc[rows, :] += mm(one_hot(proc_lanes[j], u * m, m), table1[u])
            return c

        lax.fori_loop(0, degree, edge, 0)
        return carry

    lax.fori_loop(0, UNITS - 1, proc_unit, 0)
    last1()
    pre[...] = jnp.zeros_like(pre)

    def last_edge(j, c):
        rows = proc_rows(j)
        full = acc[rows, :] + mm(one_hot(proc_lanes[j], (UNITS - 1) * m, m), table1[UNITS - 1])
        pre[...] += silu(full)
        return c

    lax.fori_loop(0, degree, last_edge, 0)
    for q in range(QUARTERS):
        rows = pl.ds(q * quarter, quarter)
        upd = own_c[rows, :] + mm(pre[rows, :].astype(BF16), weight("w_proc_agg"))
        h = (mesh_h[rows, :].astype(F32) + silu(upd)).astype(BF16)
        table2[U_OWN, rows, :] = mm(h, weight("w_dec_send")).astype(BF16)
        start2(q)

    for name in ("w_dec_recv", "w_grid_self", "w_grid_agg", "w_grid_out"):
        fetches[name].wait()

    def cell_block(b):
        return pl.ds(pl.multiple_of(b * wide, wide), wide)

    def second(b):
        return pl.ds(pl.multiple_of(cells + b * wide, wide), wide)

    def first_edges(b, c):
        rows = cell_block(b)
        h = grid_h[rows, :]
        recv = mm(h, weight("w_dec_recv"))
        cols = cell_cols[rows, :]
        acc[second(b), :] = recv + cols[:, 5:6] * w_dec_dist[...]
        near = recv + cols[:, 4:5] * w_dec_dist[...]
        near = near + mm(one_hot(key0_lanes[rows, :], 0, m), table2[U_OWN])
        acc[rows, :] = silu(near)
        u_buf[rows, :] = mm(h, weight("w_grid_self"))
        return c

    lax.fori_loop(0, cells // wide, first_edges, 0)

    def dec_unit(u, carry):
        before2(u)

        def edge(b, c):
            acc[second(b), :] += mm(one_hot(key1_lanes[cell_block(b), :], u * m, m), table2[u])
            return c

        lax.fori_loop(0, cells // wide, edge, 0)
        return carry

    lax.fori_loop(1, UNITS - 1, dec_unit, 0)
    last2()

    def finish_cells(b, c):
        rows = cell_block(b)
        far = acc[second(b), :] + mm(
            one_hot(key1_lanes[rows, :], (UNITS - 1) * m, m), table2[UNITS - 1]
        )
        agg = (acc[rows, :] + silu(far)).astype(BF16)
        z = silu(u_buf[rows, :] + mm(agg, weight("w_grid_agg"))).astype(BF16)
        change = lax.dot_general(
            w_out[...], z, (((1,), (1,)), ((), ())), preferred_element_type=F32
        )
        out[:, rows] = (grid_t[:, rows].astype(F32) + change).astype(BF16)
        return c

    lax.fori_loop(0, cells // wide, finish_cells, 0)

    for side in range(2):
        for q in range(QUARTERS):
            enc_x(side, q).wait_send()
            enc_side(side, q).wait_send()
        enc_p(side).wait_send()
        enc_c(side).wait_send()
    finish1()
    finish2()


SQUARE = (
    "w_enc_src",
    "w_mesh_self",
    "w_mesh_agg",
    "w_proc_send",
    "w_proc_recv",
    "w_proc_self",
    "w_proc_agg",
    "w_dec_send",
    "w_dec_recv",
    "w_grid_self",
    "w_grid_agg",
)
WEIGHTS = ("w_grid_in",) + SQUARE + ("w_grid_out",)


def shards(
    grid_in,
    mesh_emb,
    enc_dest,
    enc_node,
    enc_dist,
    dec_dist,
    mesh_src,
    proc_dist,
    w_grid_in,
    w_enc_src,
    w_enc_dist,
    w_mesh_self,
    w_mesh_agg,
    w_proc_send,
    w_proc_recv,
    w_proc_dist,
    w_proc_self,
    w_proc_agg,
    w_dec_send,
    w_dec_recv,
    w_dec_dist,
    w_grid_self,
    w_grid_agg,
    w_grid_out,
):
    n_lat, n_lon = lax.axis_size("lat"), lax.axis_size("lon")
    cells, variables = grid_in.shape
    m, width = mesh_emb.shape
    degree = mesh_src.shape[1]
    local = locals()
    hbm = [local[name] for name in WEIGHTS[:-1]] + [w_grid_out.T]
    vmem = pl.BlockSpec(memory_space=pltpu.VMEM)
    any_space = pl.BlockSpec(memory_space=pl.ANY)
    rows = max(degree * m, 2 * cells)
    out = pl.pallas_call(
        functools.partial(kernel, n_lat, n_lon, WEIGHTS),
        out_shape=jax.ShapeDtypeStruct((variables, cells), BF16),
        in_specs=[vmem] * 11 + [any_space] * len(WEIGHTS),
        out_specs=vmem,
        scratch_shapes=[
            pltpu.VMEM((len(SQUARE), width, width), BF16),
            pltpu.VMEM((variables, width), BF16),
            pltpu.VMEM((variables, width), BF16),
            pltpu.VMEM((8, cells), F32),
            pltpu.VMEM((8, cells), I32),
            pltpu.VMEM((cells, 8), F32),
            pltpu.VMEM((cells, 128), I32),
            pltpu.VMEM((cells, 128), I32),
            pltpu.VMEM((degree, m, 128), I32),
            pltpu.VMEM((m, degree), F32),
            pltpu.VMEM((cells, width), BF16),
            pltpu.VMEM((2, cells, width), BF16),
            pltpu.VMEM((8, m, width), BF16),
            pltpu.VMEM((8, m, width), BF16),
            pltpu.VMEM((2, m, width), BF16),
            pltpu.VMEM((m, width), F32),
            pltpu.VMEM((m, width), F32),
            pltpu.VMEM((m, width), BF16),
            pltpu.VMEM((UNITS, m, width), BF16),
            pltpu.VMEM((UNITS, m, width), BF16),
            pltpu.VMEM((rows, width), F32),
            pltpu.VMEM((cells, width), F32),
            pltpu.SemaphoreType.DMA((len(WEIGHTS),)),
            pltpu.SemaphoreType.DMA((ENC_SEMS,)),
            pltpu.SemaphoreType.DMA((ENC_SEMS,)),
            pltpu.SemaphoreType.DMA((HALO_SEMS,)),
            pltpu.SemaphoreType.DMA((HALO_SEMS,)),
            pltpu.SemaphoreType.DMA((HALO_SEMS,)),
            pltpu.SemaphoreType.DMA((HALO_SEMS,)),
        ],
        compiler_params=pltpu.CompilerParams(
            collective_id=0, has_side_effects=True, vmem_limit_bytes=67_000_000
        ),
    )(
        grid_in.T,
        mesh_emb,
        enc_dest.T,
        enc_node.T,
        enc_dist.T,
        dec_dist.T,
        mesh_src.T,
        proc_dist.T,
        w_enc_dist.reshape(1, width),
        w_proc_dist.reshape(1, width),
        w_dec_dist.reshape(1, width),
        *hbm,
    )
    return out.T


def solution(mesh):
    split = P(("lat", "lon"), None)
    in_specs = (split,) * 8 + (P(),) * 16
    return jax.shard_map(shards, mesh=mesh, in_specs=in_specs, out_specs=split, check_vma=False)
```

```python
import functools

import jax
import jax.numpy as jnp
from jax import lax
from jax.experimental import pallas as pl
from jax.experimental.pallas import tpu as pltpu
from jax.sharding import PartitionSpec as P

BF16 = jnp.bfloat16
F32 = jnp.float32
I32 = jnp.int32
QUARTERS = 4
LAST = QUARTERS - 1
ORDER = (LAST,) + tuple(range(LAST))

PARTNER, CROSS, LEFT, RIGHT = range(4)

XL, XR, PL_, PR, OL, OR, XC, PC = range(8)

U_OWN, U_PART, U_CROSS = 0, 1, 3
U_SIDE = {"own": (2, 5), "part": (4, 7), "cross": (6, 8)}
UNITS = 9

ENC_SEMS = 2 * QUARTERS + 2 + 2 * QUARTERS + 2
HALO_SEMS = 8 * QUARTERS


def silu_of_half(h):
    return h + h * jnp.tanh(h)


def silu(v):
    return silu_of_half(0.5 * v)


def mm(a, b):
    return jnp.dot(a, b, preferred_element_type=F32)


def one_hot(keys, base, width):
    lane = lax.broadcasted_iota(I32, keys.shape, 1)
    shifted = keys - base
    pieces = [
        jnp.where(shifted == lane + g * 128, 1.0, 0.0).astype(BF16) for g in range(width // 128)
    ]
    return jnp.concatenate(pieces, axis=1)


def kernel(
    n_lat,
    n_lon,
    weights,
    grid_t,
    emb,
    dest,
    node,
    enc_d,
    dec_d,
    src,
    proc_d,
    w_enc_dist,
    w_proc_dist,
    w_dec_dist,
    *refs,
):
    hbm = dict(zip(weights, refs[: len(weights)]))
    (
        out,
        wv_all,
        w_in,
        w_out,
        cell_keys,
        cell_rows,
        cell_cols,
        key1_lanes,
        key0_lanes,
        proc_lanes,
        proc_cols,
        grid_h,
        msg,
        sb,
        rb,
        ss,
        own_c,
        pre,
        mesh_h,
        table1,
        table2,
        acc,
        near_buf,
        far_buf,
        u_buf,
        w_sems,
        enc_send,
        enc_recv,
        h1_send,
        h1_recv,
        h2_send,
        h2_recv,
    ) = refs[len(weights) :]
    m, width = emb.shape
    cells = grid_t.shape[1]
    degree = src.shape[0]
    quarter = m // QUARTERS
    half = m // 2
    block = min(256, cells)
    wide = min(512, cells)

    lat = lax.axis_index("lat")
    lon = lax.axis_index("lon")
    core = lat % 2
    toward = 1 - 2 * core
    partner = (lat + toward, lon)
    cross = ((lat - toward + n_lat) % n_lat, lon)
    left = (lat, (lon - 1 + n_lon) % n_lon)
    right = (lat, (lon + 1) % n_lon)
    peers = (partner, cross, left, right)

    square = [name for name in weights if name not in ("w_grid_in", "w_grid_out")]
    w_at = {name: wv_all.at[i] for i, name in enumerate(square)}
    w_at["w_grid_in"] = w_in
    w_at["w_grid_out"] = w_out
    fetches = {
        name: pltpu.make_async_copy(hbm[name], w_at[name], w_sems.at[i])
        for i, name in enumerate(weights)
    }
    for name in weights:
        fetches[name].start()
    barrier = pltpu.get_barrier_semaphore()
    for peer in peers:
        pl.semaphore_signal(
            barrier, inc=1, device_id=peer, device_id_type=pl.DeviceIdType.MESH
        )

    def weight(name):
        return w_at[name][...]

    def remote(src_ref, dst_ref, send, recv, i, peer):
        return pltpu.make_async_remote_copy(
            src_ref=src_ref,
            dst_ref=dst_ref,
            send_sem=send.at[i],
            recv_sem=recv.at[i],
            device_id=peers[peer],
            device_id_type=pl.DeviceIdType.MESH,
        )

    shift = m.bit_length() - 1
    lon_shift = n_lon.bit_length() - 1

    def places(patch):
        d_row = (patch >> lon_shift) - lat
        side = ((patch & (n_lon - 1)) - lon + 1) & (n_lon - 1)
        return d_row == 0, d_row == toward, side

    def gather_key(patch, at):
        own, part, side = places(patch)
        upper = (at >= half).astype(I32)
        centre = jnp.where(own, U_OWN, jnp.where(part, U_PART, U_CROSS)) * m + at
        first = jnp.where(own, U_SIDE["own"][0], jnp.where(part, U_SIDE["part"][0], U_SIDE["cross"][0]))
        second = jnp.where(own, U_SIDE["own"][1], jnp.where(part, U_SIDE["part"][1], U_SIDE["cross"][1]))
        unit = jnp.where(upper == 1, second, first)
        beside = unit * m + jnp.where(side == 2, half, 0) + at - upper * half
        return jnp.where(side == 1, centre, beside)

    patch1 = dest[1:2, :]
    node1 = node[1:2, :]
    own1, part1, side1 = places(patch1)
    slot_l = jnp.where(own1, OL, jnp.where(part1, PL_, XL))
    slot_r = jnp.where(own1, OR, jnp.where(part1, PR, XR))
    slot_c = jnp.where(part1, PC, XC)
    slot = jnp.where(side1 == 0, slot_l, jnp.where(side1 == 2, slot_r, slot_c))
    cell_rows[0:1, :] = slot * m + node1
    cell_rows[1:2, :] = node[0:1, :]
    cell_keys[...] = jnp.zeros_like(cell_keys)
    cell_keys[0:1, :] = node[0:1, :].astype(F32)
    cell_keys[1:2, :] = gather_key(patch1, node1).astype(F32)
    cell_keys[2:4, :] = enc_d[...]
    cell_keys[4:6, :] = dec_d[...]
    cell_cols[...] = jnp.transpose(cell_keys[...])
    mesh_key = gather_key(src[...] >> shift, src[...] & (m - 1)).astype(F32)
    mesh_key_t = jnp.transpose(mesh_key)
    proc_cols[...] = jnp.transpose(proc_d[...])
    for j in range(degree):
        lanes = jnp.broadcast_to(mesh_key_t[:, j : j + 1], (m, 128)).astype(I32)
        for q in range(QUARTERS):
            proc_lanes[pl.ds((q * degree + j) * quarter, quarter), :] = lanes[
                q * quarter : (q + 1) * quarter
            ]

    fetches["w_grid_in"].wait()
    fetches["w_enc_src"].wait()

    def embed(b, carry):
        rows = pl.ds(pl.multiple_of(b * block, block), block)
        part = grid_t[:, rows]
        h = silu(
            lax.dot_general(part, w_in[...], (((0,), (0,)), ((), ())), preferred_element_type=F32)
        ).astype(BF16)
        grid_h[rows, :] = h
        e = 0.5 * mm(h, weight("w_enc_src"))
        cols = cell_cols[rows, :]
        half_dist = 0.5 * w_enc_dist[...]
        for k in range(2):
            msg[k, rows, :] = silu_of_half(e + cols[:, 2 + k : 3 + k] * half_dist).astype(BF16)
        key0_lanes[rows, :] = jnp.broadcast_to(cols[:, 0:1], (block, 128)).astype(I32)
        key1_lanes[rows, :] = jnp.broadcast_to(cols[:, 1:2], (block, 128)).astype(I32)
        return carry

    lax.fori_loop(0, cells // block, embed, 0)
    pl.semaphore_wait(barrier, 4)

    def enc_x(side, q):
        rows = pl.ds(q * quarter, quarter)
        return remote(
            sb.at[side, rows], rb.at[side, rows], enc_send, enc_recv, 2 * q + side, CROSS
        )

    def enc_p(side):
        return remote(
            sb.at[2 + side], rb.at[2 + side], enc_send, enc_recv, 2 * QUARTERS + side, PARTNER
        )

    def enc_side(side, q):
        rows = pl.ds(q * quarter, quarter)
        return remote(
            ss.at[side, rows],
            rb.at[4 + side, rows],
            enc_send,
            enc_recv,
            2 * QUARTERS + 2 + 2 * q + side,
            LEFT if side == 0 else RIGHT,
        )

    def enc_c(which):
        return remote(
            sb.at[XC + which],
            rb.at[XC + which],
            enc_send,
            enc_recv,
            4 * QUARTERS + 2 + which,
            CROSS if which == 0 else PARTNER,
        )

    def relay_sums(q):
        rows = pl.ds(q * quarter, quarter)
        for side in range(2):
            enc_x(side, q).wait_recv()
            if q == 0:
                enc_p(side).wait_recv()
            total = (
                sb[4 + side, rows, :].astype(F32)
                + rb[side, rows, :].astype(F32)
                + rb[2 + side, rows, :].astype(F32)
            )
            ss[side, rows, :] = total.astype(BF16)
        for side in range(2):
            enc_side(side, q).start()

    def scatter(row, base, which, rows):
        keys = cell_rows[row : row + 1, :] - base
        sel = jnp.where(lax.broadcasted_iota(I32, (rows, cells), 0) == keys, 1.0, 0.0).astype(BF16)
        return mm(sel, msg[which])

    def cell_block(b):
        return pl.ds(b * wide, wide)

    def cell_terms(blocks):
        for b in blocks:
            rows = cell_block(b)
            h = grid_h[rows, :]
            recv = mm(h, weight("w_dec_recv"))
            cols = cell_cols[rows, :]
            near_buf[rows, :] = recv + cols[:, 4:5] * w_dec_dist[...]
            far_buf[rows, :] = recv + cols[:, 5:6] * w_dec_dist[...]
            u_buf[rows, :] = mm(h, weight("w_grid_self"))

    for upper in range(2):
        for side in range(2):
            part = scatter(0, side * m + upper * half, 1, half)
            sb[side, pl.ds(upper * half, half), :] = part.astype(BF16)
        for q in range(2 * upper, 2 * upper + 2):
            for side in range(2):
                enc_x(side, q).start()

    def partial_step(s, carry):
        sb[s] = scatter(0, s * m, 1, m).astype(BF16)

        @pl.when(s == PR)
        def _():
            for side in range(2):
                enc_p(side).start()

        @pl.when(s == OR)
        def _():
            relay_sums(0)

        @pl.when(s == XC)
        def _():
            enc_c(0).start()

        @pl.when(s == PC)
        def _():
            enc_c(1).start()

        return carry

    lax.fori_loop(2, 8, partial_step, 0)
    relay_sums(1)
    own_c[...] = scatter(1, 0, 0, m)
    fetches["w_dec_recv"].wait()
    fetches["w_grid_self"].wait()
    blocks = cells // wide
    cell_terms(range(0, blocks // 2))
    relay_sums(2)
    cell_terms(range(blocks // 2, blocks))
    relay_sums(3)

    fetches["w_mesh_self"].wait()
    fetches["w_mesh_agg"].wait()
    fetches["w_proc_send"].wait()
    pre[...] = mm(emb[...], weight("w_mesh_self"))
    enc_c(0).wait_recv()
    enc_c(1).wait_recv()

    def halo(table, send, recv):
        def own(q, peer):
            src_ref = table.at[U_OWN, pl.ds(q * quarter, quarter)]
            if peer == PARTNER:
                dst = table.at[U_PART, pl.ds(q * quarter, quarter)]
            elif peer == CROSS:
                dst = table.at[U_CROSS, pl.ds(q * quarter, quarter)]
            else:
                dst = side_rows("own", 1 if peer == LEFT else 0, q)
            return remote(src_ref, dst, send, recv, 4 * q + peer, peer)

        def side_rows(owner, side, q):
            unit = U_SIDE[owner][q // 2]
            return table.at[unit, pl.ds(side * half + (q % 2) * quarter, quarter)]

        def forward(side, q, peer):
            dst = side_rows("part" if peer == PARTNER else "cross", side, q)
            index = 4 * QUARTERS + 4 * q + 2 * side + peer
            if peer == CROSS and q == LAST:
                src_ref = table.at[U_CROSS, pl.ds(q * quarter, quarter)]
                return remote(src_ref, dst, send, recv, index, RIGHT if side == 0 else LEFT)
            return remote(side_rows("own", side, q), dst, send, recv, index, peer)

        def start_own(q):
            for peer in (LEFT, RIGHT, CROSS, PARTNER):
                own(q, peer).start()

        def pass_on(q):
            own(q, RIGHT).wait_recv()
            own(q, LEFT).wait_recv()
            for side in range(2):
                if q != LAST:
                    forward(side, q, CROSS).start()
                forward(side, q, PARTNER).start()

        def turn_corner():
            own(LAST, CROSS).wait_recv()
            for side in range(2):
                forward(side, LAST, CROSS).start()

        def wait_forwarded(peer, quarters):
            for q in quarters:
                for side in range(2):
                    forward(side, q, peer).wait_recv()

        def before(u):
            @pl.when(u == 2)
            def _():
                pass_on(1)

            @pl.when(u == 3)
            def _():
                for q in range(QUARTERS):
                    if q != LAST:
                        own(q, CROSS).wait_recv()

            @pl.when(u == 4)
            def _():
                pass_on(2)
                wait_forwarded(PARTNER, (0, 1))

            @pl.when(u == 5)
            def _():
                pass_on(LAST)

            @pl.when(u == 6)
            def _():
                wait_forwarded(CROSS, (0, 1))

        def before_partner():
            for q in range(QUARTERS):
                own(q, PARTNER).wait_recv()

        def before_last(units):
            if 6 in units:
                wait_forwarded(CROSS, (0, 1))
            wait_forwarded(PARTNER, (2, 3))
            wait_forwarded(CROSS, (2, 3))

        def finish():
            for q in range(QUARTERS):
                for peer in range(4):
                    own(q, peer).wait_send()
                for side in range(2):
                    for peer in (PARTNER, CROSS):
                        forward(side, q, peer).wait_send()

        return start_own, before_partner, pass_on, turn_corner, before, before_last, finish

    start1, partner1, pass1, turn1, before1, last1, finish1 = halo(table1, h1_send, h1_recv)
    start2, partner2, pass2, turn2, before2, last2, finish2 = halo(table2, h2_send, h2_recv)

    for q in ORDER:
        rows = pl.ds(q * quarter, quarter)
        for side in range(2):
            enc_side(side, q).wait_recv()
        total = own_c[rows, :]
        for i in range(4, 8):
            total = total + rb[i, rows, :].astype(F32)
        upd = pre[rows, :] + mm(total.astype(BF16), weight("w_mesh_agg"))
        h = (emb[rows, :].astype(F32) + silu(upd)).astype(BF16)
        mesh_h[rows, :] = h
        table1[U_OWN, rows, :] = mm(h, weight("w_proc_send")).astype(BF16)
        start1(q)

    for name in ("w_proc_recv", "w_proc_self", "w_proc_agg", "w_dec_send"):
        fetches[name].wait()
    pre[...] = mm(mesh_h[...], weight("w_proc_recv"))
    own_c[...] = mm(mesh_h[...], weight("w_proc_self"))
    group = 2 * QUARTERS
    edge_rows = degree * m // group
    per_group = edge_rows // quarter

    def edges(g):
        return pl.ds(g * edge_rows, edge_rows)

    def units(table, first, last):
        return table[first:last].reshape((last - first) * m, width)

    partner1()
    for g in range(group):
        parts = []
        for e in range(g * per_group, (g + 1) * per_group):
            rows = pl.ds(e // degree * quarter, quarter)
            j = e % degree
            parts.append(pre[rows, :] + proc_cols[rows, j : j + 1] * w_proc_dist[...])
        base = jnp.concatenate(parts, axis=0)
        acc[edges(g), :] = base + mm(
            one_hot(proc_lanes[edges(g), :], 0, 2 * m), units(table1, 0, 2)
        )
    pass1(0)
    turn1()

    def proc_unit(u, carry):
        before1(u)
        for g in range(group):
            acc[edges(g), :] += mm(one_hot(proc_lanes[edges(g), :], u * m, m), table1[u])
        return carry

    lax.fori_loop(2, 6, proc_unit, 0)
    last1((6, 7, 8))
    for q in ORDER:
        rows = pl.ds(q * quarter, quarter)
        agg = None
        for g in range(q * degree // per_group, (q + 1) * degree // per_group):
            full = acc[edges(g), :] + mm(
                one_hot(proc_lanes[edges(g), :], 6 * m, 3 * m), units(table1, 6, 9)
            )
            messages = silu(full)
            for i in range(per_group):
                one = messages[i * quarter : (i + 1) * quarter]
                agg = one if agg is None else agg + one
        upd = own_c[rows, :] + mm(agg.astype(BF16), weight("w_proc_agg"))
        h = (mesh_h[rows, :].astype(F32) + silu(upd)).astype(BF16)
        table2[U_OWN, rows, :] = mm(h, weight("w_dec_send")).astype(BF16)
        start2(q)

    for b in range(cells // wide):
        rows = cell_block(b)
        near = near_buf[rows, :] + mm(one_hot(key0_lanes[rows, :], 0, m), table2[U_OWN])
        near_buf[rows, :] = silu(near)
    partner2()
    pass2(0)
    turn2()
    for b in range(cells // wide):
        rows = cell_block(b)
        far_buf[rows, :] += mm(one_hot(key1_lanes[rows, :], m, m), table2[U_PART])

    def dec_unit(u, carry):
        before2(u)
        for b in range(cells // wide):
            rows = cell_block(b)
            far_buf[rows, :] += mm(one_hot(key1_lanes[rows, :], u * m, m), table2[u])
        return carry

    lax.fori_loop(2, 7, dec_unit, 0)
    last2((7, 8))
    fetches["w_grid_agg"].wait()
    fetches["w_grid_out"].wait()
    for b in range(cells // wide):
        rows = cell_block(b)
        far = far_buf[rows, :] + mm(
            one_hot(key1_lanes[rows, :], 7 * m, 2 * m), units(table2, 7, 9)
        )
        agg = (near_buf[rows, :] + silu(far)).astype(BF16)
        z = silu(u_buf[rows, :] + mm(agg, weight("w_grid_agg"))).astype(BF16)
        change = lax.dot_general(
            w_out[...], z, (((1,), (1,)), ((), ())), preferred_element_type=F32
        )
        out[:, rows] = (grid_t[:, rows].astype(F32) + change).astype(BF16)

    for side in range(2):
        for q in range(QUARTERS):
            enc_x(side, q).wait_send()
            enc_side(side, q).wait_send()
        enc_p(side).wait_send()
        enc_c(side).wait_send()
    finish1()
    finish2()


SQUARE = (
    "w_enc_src",
    "w_mesh_self",
    "w_mesh_agg",
    "w_proc_send",
    "w_proc_recv",
    "w_proc_self",
    "w_proc_agg",
    "w_dec_send",
    "w_dec_recv",
    "w_grid_self",
    "w_grid_agg",
)
WEIGHTS = ("w_grid_in",) + SQUARE + ("w_grid_out",)


def shards(
    grid_in,
    mesh_emb,
    enc_dest,
    enc_node,
    enc_dist,
    dec_dist,
    mesh_src,
    proc_dist,
    w_grid_in,
    w_enc_src,
    w_enc_dist,
    w_mesh_self,
    w_mesh_agg,
    w_proc_send,
    w_proc_recv,
    w_proc_dist,
    w_proc_self,
    w_proc_agg,
    w_dec_send,
    w_dec_recv,
    w_dec_dist,
    w_grid_self,
    w_grid_agg,
    w_grid_out,
):
    n_lat, n_lon = lax.axis_size("lat"), lax.axis_size("lon")
    cells, variables = grid_in.shape
    m, width = mesh_emb.shape
    degree = mesh_src.shape[1]
    local = locals()
    hbm = [local[name] for name in WEIGHTS[:-1]] + [w_grid_out.T]
    vmem = pl.BlockSpec(memory_space=pltpu.VMEM)
    any_space = pl.BlockSpec(memory_space=pl.ANY)
    out = pl.pallas_call(
        functools.partial(kernel, n_lat, n_lon, WEIGHTS),
        out_shape=jax.ShapeDtypeStruct((variables, cells), BF16),
        in_specs=[vmem] * 11 + [any_space] * len(WEIGHTS),
        out_specs=vmem,
        scratch_shapes=[
            pltpu.VMEM((len(SQUARE), width, width), BF16),
            pltpu.VMEM((variables, width), BF16),
            pltpu.VMEM((variables, width), BF16),
            pltpu.VMEM((8, cells), F32),
            pltpu.VMEM((8, cells), I32),
            pltpu.VMEM((cells, 8), F32),
            pltpu.VMEM((cells, 128), I32),
            pltpu.VMEM((cells, 128), I32),
            pltpu.VMEM((degree * m, 128), I32),
            pltpu.VMEM((m, degree), F32),
            pltpu.VMEM((cells, width), BF16),
            pltpu.VMEM((2, cells, width), BF16),
            pltpu.VMEM((8, m, width), BF16),
            pltpu.VMEM((8, m, width), BF16),
            pltpu.VMEM((2, m, width), BF16),
            pltpu.VMEM((m, width), F32),
            pltpu.VMEM((m, width), F32),
            pltpu.VMEM((m, width), BF16),
            pltpu.VMEM((UNITS, m, width), BF16),
            pltpu.VMEM((UNITS, m, width), BF16),
            pltpu.VMEM((degree * m, width), F32),
            pltpu.VMEM((cells, width), F32),
            pltpu.VMEM((cells, width), F32),
            pltpu.VMEM((cells, width), F32),
            pltpu.SemaphoreType.DMA((len(WEIGHTS),)),
            pltpu.SemaphoreType.DMA((ENC_SEMS,)),
            pltpu.SemaphoreType.DMA((ENC_SEMS,)),
            pltpu.SemaphoreType.DMA((HALO_SEMS,)),
            pltpu.SemaphoreType.DMA((HALO_SEMS,)),
            pltpu.SemaphoreType.DMA((HALO_SEMS,)),
            pltpu.SemaphoreType.DMA((HALO_SEMS,)),
        ],
        compiler_params=pltpu.CompilerParams(
            collective_id=0, has_side_effects=True, vmem_limit_bytes=67_000_000
        ),
    )(
        grid_in.T,
        mesh_emb,
        enc_dest.T,
        enc_node.T,
        enc_dist.T,
        dec_dist.T,
        mesh_src.T,
        proc_dist.T,
        w_enc_dist.reshape(1, width),
        w_proc_dist.reshape(1, width),
        w_dec_dist.reshape(1, width),
        *hbm,
    )
    return out.T


def solution(mesh):
    split = P(("lat", "lon"), None)
    in_specs = (split,) * 8 + (P(),) * 16
    return jax.shard_map(shards, mesh=mesh, in_specs=in_specs, out_specs=split, check_vma=False)
```

```python
import functools

import jax
import jax.numpy as jnp
from jax import lax
from jax.experimental import pallas as pl
from jax.experimental.pallas import tpu as pltpu
from jax.sharding import PartitionSpec as P

BF16 = jnp.bfloat16
F32 = jnp.float32
I32 = jnp.int32
QUARTERS = 4
LAST = QUARTERS - 1

PARTNER, CROSS, LEFT, RIGHT = range(4)

XL, XR, PL_, PR, OL, OR, XC, PC = range(8)

U_OWN, U_PART, U_CROSS = 0, 1, 3
U_SIDE = {"own": (2, 5), "part": (4, 7), "cross": (6, 8)}
UNITS = 9

ENC_SEMS = 5 * QUARTERS + 3
HALO_SEMS = 8 * QUARTERS


def silu_of_half(h):
    return h + h * jnp.tanh(h)


def silu(v):
    return silu_of_half(0.5 * v)


def mm(a, b):
    return jnp.dot(a, b, preferred_element_type=F32)


def one_hot(keys, base, width):
    lane = lax.broadcasted_iota(I32, keys.shape, 1)
    shifted = keys - base
    pieces = [
        jnp.where(shifted == lane + g * 128, 1.0, 0.0).astype(BF16) for g in range(width // 128)
    ]
    return jnp.concatenate(pieces, axis=1)


def kernel(
    n_lat,
    n_lon,
    weights,
    grid_t,
    dest,
    node,
    enc_d,
    dec_d,
    src,
    proc_d,
    w_enc_dist,
    w_proc_dist,
    w_dec_dist,
    *refs,
):
    hbm = dict(zip(weights, refs[: len(weights)]))
    (
        out,
        emb,
        wv_all,
        w_in,
        w_out,
        cell_keys,
        cell_rows,
        cell_cols,
        key1_lanes,
        key0_lanes,
        proc_lanes,
        proc_cols,
        grid_h,
        msg,
        sb,
        rb,
        ss,
        own_c,
        pre,
        mesh_h,
        table1,
        table2,
        acc,
        near_buf,
        far_buf,
        u_buf,
        w_sems,
        enc_send,
        enc_recv,
        h1_send,
        h1_recv,
        h2_send,
        h2_recv,
    ) = refs[len(weights) :]
    m, width = emb.shape
    cells = grid_t.shape[1]
    degree = src.shape[0]
    quarter = m // QUARTERS
    half = m // 2
    block = min(256, cells)
    wide = min(512, cells)

    lat = lax.axis_index("lat")
    lon = lax.axis_index("lon")
    core = lat % 2
    toward = 1 - 2 * core
    partner = (lat + toward, lon)
    cross = ((lat - toward + n_lat) % n_lat, lon)
    left = (lat, (lon - 1 + n_lon) % n_lon)
    right = (lat, (lon + 1) % n_lon)
    peers = (partner, cross, left, right)

    square = [name for name in weights if name in SQUARE]
    w_at = {name: wv_all.at[i] for i, name in enumerate(square)}
    w_at["w_grid_in"] = w_in
    w_at["mesh_emb"] = emb
    w_at["w_grid_out"] = w_out
    fetches = {
        name: pltpu.make_async_copy(hbm[name], w_at[name], w_sems.at[i])
        for i, name in enumerate(weights)
    }
    for name in weights:
        fetches[name].start()
    barrier = pltpu.get_barrier_semaphore()
    for peer in peers:
        pl.semaphore_signal(
            barrier, inc=1, device_id=peer, device_id_type=pl.DeviceIdType.MESH
        )

    def weight(name):
        return w_at[name][...]

    def remote(src_ref, dst_ref, send, recv, i, peer):
        return pltpu.make_async_remote_copy(
            src_ref=src_ref,
            dst_ref=dst_ref,
            send_sem=send.at[i],
            recv_sem=recv.at[i],
            device_id=peers[peer],
            device_id_type=pl.DeviceIdType.MESH,
        )

    shift = m.bit_length() - 1
    lon_shift = n_lon.bit_length() - 1

    def places(patch):
        d_row = (patch >> lon_shift) - lat
        side = ((patch & (n_lon - 1)) - lon + 1) & (n_lon - 1)
        return d_row == 0, d_row == toward, side

    def gather_key(patch, at):
        own, part, side = places(patch)
        upper = (at >= half).astype(I32)
        centre = jnp.where(own, U_OWN, jnp.where(part, U_PART, U_CROSS)) * m + at
        first = jnp.where(own, U_SIDE["own"][0], jnp.where(part, U_SIDE["part"][0], U_SIDE["cross"][0]))
        second = jnp.where(own, U_SIDE["own"][1], jnp.where(part, U_SIDE["part"][1], U_SIDE["cross"][1]))
        unit = jnp.where(upper == 1, second, first)
        beside = unit * m + jnp.where(side == 2, half, 0) + at - upper * half
        return jnp.where(side == 1, centre, beside)

    patch1 = dest[1:2, :]
    node1 = node[1:2, :]
    own1, part1, side1 = places(patch1)
    slot_l = jnp.where(own1, OL, jnp.where(part1, PL_, XL))
    slot_r = jnp.where(own1, OR, jnp.where(part1, PR, XR))
    slot_c = jnp.where(part1, PC, XC)
    slot = jnp.where(side1 == 0, slot_l, jnp.where(side1 == 2, slot_r, slot_c))
    cell_rows[0:1, :] = slot * m + node1
    cell_rows[1:2, :] = node[0:1, :]
    cell_keys[...] = jnp.zeros_like(cell_keys)
    cell_keys[0:1, :] = node[0:1, :].astype(F32)
    cell_keys[1:2, :] = gather_key(patch1, node1).astype(F32)
    cell_keys[2:4, :] = enc_d[...]
    cell_keys[4:6, :] = dec_d[...]
    cell_cols[...] = jnp.transpose(cell_keys[...])
    mesh_key = gather_key(src[...] >> shift, src[...] & (m - 1)).astype(F32)
    mesh_key_t = jnp.transpose(mesh_key)
    proc_cols[...] = jnp.transpose(proc_d[...])
    for j in range(degree):
        lanes = jnp.broadcast_to(mesh_key_t[:, j : j + 1], (m, 128)).astype(I32)
        for q in range(QUARTERS):
            proc_lanes[pl.ds((q * degree + j) * quarter, quarter), :] = lanes[
                q * quarter : (q + 1) * quarter
            ]

    fetches["w_grid_in"].wait()
    fetches["w_enc_src"].wait()
    w_in[...] = w_in[...] * 0.5
    w_at["w_enc_src"][...] = weight("w_enc_src") * 0.5
    half_dist = 0.5 * w_enc_dist[...]

    def embed(b, carry):
        rows = pl.ds(pl.multiple_of(b * block, block), block)
        part = grid_t[:, rows]
        h = silu_of_half(
            lax.dot_general(part, w_in[...], (((0,), (0,)), ((), ())), preferred_element_type=F32)
        ).astype(BF16)
        grid_h[rows, :] = h
        e = mm(h, weight("w_enc_src"))
        cols = cell_cols[rows, :]
        for k in range(2):
            msg[k, rows, :] = silu_of_half(e + cols[:, 2 + k : 3 + k] * half_dist).astype(BF16)
        key0_lanes[rows, :] = jnp.broadcast_to(cols[:, 0:1], (block, 128)).astype(I32)
        key1_lanes[rows, :] = jnp.broadcast_to(cols[:, 1:2], (block, 128)).astype(I32)
        return carry

    lax.fori_loop(0, cells // block, embed, 0)
    pl.semaphore_wait(barrier, 4)

    def enc_x(side, q):
        rows = pl.ds(q * quarter, quarter)
        return remote(
            sb.at[side, rows], rb.at[side, rows], enc_send, enc_recv, 2 * q + side, CROSS
        )

    def enc_p(side):
        return remote(
            sb.at[2 + side], rb.at[2 + side], enc_send, enc_recv, 2 * QUARTERS + side, PARTNER
        )

    def enc_side(side, q):
        rows = pl.ds(q * quarter, quarter)
        return remote(
            ss.at[side, rows],
            rb.at[4 + side, rows],
            enc_send,
            enc_recv,
            2 * QUARTERS + 2 + 2 * q + side,
            LEFT if side == 0 else RIGHT,
        )

    def enc_cx(q):
        rows = pl.ds(q * quarter, quarter)
        return remote(
            sb.at[XC, rows], rb.at[XC, rows], enc_send, enc_recv, 4 * QUARTERS + 2 + q, CROSS
        )

    def enc_cp():
        return remote(sb.at[PC], rb.at[PC], enc_send, enc_recv, 5 * QUARTERS + 2, PARTNER)

    def relay_sums(q):
        rows = pl.ds(q * quarter, quarter)
        for side in range(2):
            enc_x(side, q).wait_recv()
            if q == 0:
                enc_p(side).wait_recv()
            total = (
                sb[4 + side, rows, :].astype(F32)
                + rb[side, rows, :].astype(F32)
                + rb[2 + side, rows, :].astype(F32)
            )
            ss[side, rows, :] = total.astype(BF16)
        for side in range(2):
            enc_side(side, q).start()

    def scatter(row, base, which, rows):
        keys = cell_rows[row : row + 1, :] - base
        sel = jnp.where(lax.broadcasted_iota(I32, (rows, cells), 0) == keys, 1.0, 0.0).astype(BF16)
        return mm(sel, msg[which])

    def cell_block(b):
        return pl.ds(b * wide, wide)

    def cell_terms(blocks):
        for b in blocks:
            rows = cell_block(b)
            h = grid_h[rows, :]
            recv = mm(h, weight("w_dec_recv"))
            cols = cell_cols[rows, :]
            near_buf[rows, :] = recv + cols[:, 4:5] * w_dec_dist[...]
            far_buf[rows, :] = recv + cols[:, 5:6] * w_dec_dist[...]
            u_buf[rows, :] = mm(h, weight("w_grid_self"))

    for upper in range(2):
        for side in range(2):
            part = scatter(0, side * m + upper * half, 1, half)
            sb[side, pl.ds(upper * half, half), :] = part.astype(BF16)
        for q in range(2 * upper, 2 * upper + 2):
            for side in range(2):
                enc_x(side, q).start()

    def partial_step(s, carry):
        sb[s] = scatter(0, s * m, 1, m).astype(BF16)

        @pl.when(s == PR)
        def _():
            for side in range(2):
                enc_p(side).start()

        @pl.when(s == OR)
        def _():
            relay_sums(0)

        @pl.when(s == XC)
        def _():
            for q in range(QUARTERS):
                enc_cx(q).start()

        @pl.when(s == PC)
        def _():
            enc_cp().start()

        return carry

    lax.fori_loop(2, 8, partial_step, 0)
    relay_sums(1)
    own_c[...] = scatter(1, 0, 0, m)
    fetches["w_dec_recv"].wait()
    fetches["w_grid_self"].wait()
    blocks = cells // wide
    cell_terms(range(0, blocks // 2))
    relay_sums(2)
    cell_terms(range(blocks // 2, blocks))
    for name in ("mesh_emb", "w_mesh_self", "w_mesh_agg", "w_proc_send"):
        fetches[name].wait()
    pre[...] = mm(emb[...], weight("w_mesh_self"))
    relay_sums(3)

    enc_cp().wait_recv()

    def halo(table, send, recv):
        def own(q, peer):
            src_ref = table.at[U_OWN, pl.ds(q * quarter, quarter)]
            if peer == PARTNER:
                dst = table.at[U_PART, pl.ds(q * quarter, quarter)]
            elif peer == CROSS:
                dst = table.at[U_CROSS, pl.ds(q * quarter, quarter)]
            else:
                dst = side_rows("own", 1 if peer == LEFT else 0, q)
            return remote(src_ref, dst, send, recv, 4 * q + peer, peer)

        def side_rows(owner, side, q):
            unit = U_SIDE[owner][q // 2]
            return table.at[unit, pl.ds(side * half + (q % 2) * quarter, quarter)]

        def forward(side, q, peer):
            dst = side_rows("part" if peer == PARTNER else "cross", side, q)
            index = 4 * QUARTERS + 4 * q + 2 * side + peer
            if peer == CROSS and q == LAST:
                src_ref = table.at[U_CROSS, pl.ds(q * quarter, quarter)]
                return remote(src_ref, dst, send, recv, index, RIGHT if side == 0 else LEFT)
            return remote(side_rows("own", side, q), dst, send, recv, index, peer)

        def start_own(q):
            for peer in (LEFT, RIGHT, CROSS, PARTNER):
                own(q, peer).start()

        def pass_on(q):
            own(q, RIGHT).wait_recv()
            own(q, LEFT).wait_recv()
            for side in range(2):
                if q != LAST:
                    forward(side, q, CROSS).start()
                forward(side, q, PARTNER).start()

        def turn_corner():
            own(LAST, CROSS).wait_recv()
            for side in range(2):
                forward(side, LAST, CROSS).start()

        def wait_forwarded(peer, quarters):
            for q in quarters:
                for side in range(2):
                    forward(side, q, peer).wait_recv()

        def before(u):
            @pl.when(u == 3)
            def _():
                pass_on(2)
                for q in range(QUARTERS):
                    if q != LAST:
                        own(q, CROSS).wait_recv()

            @pl.when(u == 4)
            def _():
                wait_forwarded(PARTNER, (0, 1))

            @pl.when(u == 5)
            def _():
                pass_on(LAST)

            @pl.when(u == 6)
            def _():
                wait_forwarded(CROSS, (0, 1))

        def before_partner():
            for q in range(QUARTERS):
                own(q, PARTNER).wait_recv()

        def before_last(units):
            if 6 in units:
                wait_forwarded(CROSS, (0, 1))
            wait_forwarded(PARTNER, (2, 3))
            wait_forwarded(CROSS, (2, 3))

        def finish():
            for q in range(QUARTERS):
                for peer in range(4):
                    own(q, peer).wait_send()
                for side in range(2):
                    for peer in (PARTNER, CROSS):
                        forward(side, q, peer).wait_send()

        return start_own, before_partner, pass_on, turn_corner, before, before_last, finish

    start1, partner1, pass1, turn1, before1, last1, finish1 = halo(table1, h1_send, h1_recv)
    start2, partner2, pass2, turn2, before2, last2, finish2 = halo(table2, h2_send, h2_recv)

    for q in range(QUARTERS):
        rows = pl.ds(q * quarter, quarter)
        for side in range(2):
            enc_side(side, q).wait_recv()
        enc_cx(q).wait_recv()
        total = own_c[rows, :]
        for i in range(4, 8):
            total = total + rb[i, rows, :].astype(F32)
        upd = pre[rows, :] + mm(total.astype(BF16), weight("w_mesh_agg"))
        h = (emb[rows, :].astype(F32) + silu(upd)).astype(BF16)
        mesh_h[rows, :] = h
        table1[U_OWN, rows, :] = mm(h, weight("w_proc_send")).astype(BF16)
        start1(q)

    for name in ("w_proc_recv", "w_proc_self", "w_proc_agg", "w_dec_send"):
        fetches[name].wait()
    pre[...] = mm(mesh_h[...], weight("w_proc_recv"))
    own_c[...] = mm(mesh_h[...], weight("w_proc_self"))
    group = 2 * QUARTERS
    edge_rows = degree * m // group
    per_group = edge_rows // quarter

    def edges(g):
        return pl.ds(g * edge_rows, edge_rows)

    def units(table, first, last):
        return table[first:last].reshape((last - first) * m, width)

    partner1()
    for g in range(group):
        if g == group // 2:
            pass1(0)
            pass1(1)
        parts = []
        for e in range(g * per_group, (g + 1) * per_group):
            rows = pl.ds(e // degree * quarter, quarter)
            j = e % degree
            parts.append(pre[rows, :] + proc_cols[rows, j : j + 1] * w_proc_dist[...])
        base = jnp.concatenate(parts, axis=0)
        acc[edges(g), :] = base + mm(
            one_hot(proc_lanes[edges(g), :], 0, 2 * m), units(table1, 0, 2)
        )
    turn1()

    def proc_unit(u, carry):
        before1(u)
        for g in range(group):
            acc[edges(g), :] += mm(one_hot(proc_lanes[edges(g), :], u * m, m), table1[u])
        return carry

    lax.fori_loop(2, 6, proc_unit, 0)
    last1((6, 7, 8))
    for q in range(QUARTERS):
        rows = pl.ds(q * quarter, quarter)
        agg = None
        for g in range(q * degree // per_group, (q + 1) * degree // per_group):
            full = acc[edges(g), :] + mm(
                one_hot(proc_lanes[edges(g), :], 6 * m, 3 * m), units(table1, 6, 9)
            )
            messages = silu(full)
            for i in range(per_group):
                one = messages[i * quarter : (i + 1) * quarter]
                agg = one if agg is None else agg + one
        upd = own_c[rows, :] + mm(agg.astype(BF16), weight("w_proc_agg"))
        h = (mesh_h[rows, :].astype(F32) + silu(upd)).astype(BF16)
        table2[U_OWN, rows, :] = mm(h, weight("w_dec_send")).astype(BF16)
        start2(q)

    for b in range(cells // wide):
        rows = cell_block(b)
        near = near_buf[rows, :] + mm(one_hot(key0_lanes[rows, :], 0, m), table2[U_OWN])
        near_buf[rows, :] = silu(near)
    partner2()
    pass2(0)
    turn2()
    pass2(1)
    for b in range(cells // wide):
        rows = cell_block(b)
        far_buf[rows, :] += mm(one_hot(key1_lanes[rows, :], m, m), table2[U_PART])

    def dec_unit(u, carry):
        before2(u)
        for b in range(cells // wide):
            rows = cell_block(b)
            far_buf[rows, :] += mm(one_hot(key1_lanes[rows, :], u * m, m), table2[u])
        return carry

    lax.fori_loop(2, 7, dec_unit, 0)
    last2((7, 8))
    fetches["w_grid_agg"].wait()
    fetches["w_grid_out"].wait()
    for b in range(cells // wide):
        rows = cell_block(b)
        far = far_buf[rows, :] + mm(
            one_hot(key1_lanes[rows, :], 7 * m, 2 * m), units(table2, 7, 9)
        )
        agg = (near_buf[rows, :] + silu(far)).astype(BF16)
        z = silu(u_buf[rows, :] + mm(agg, weight("w_grid_agg"))).astype(BF16)
        change = lax.dot_general(
            w_out[...], z, (((1,), (1,)), ((), ())), preferred_element_type=F32
        )
        out[:, rows] = (grid_t[:, rows].astype(F32) + change).astype(BF16)

    for side in range(2):
        for q in range(QUARTERS):
            enc_x(side, q).wait_send()
            enc_side(side, q).wait_send()
        enc_p(side).wait_send()
    for q in range(QUARTERS):
        enc_cx(q).wait_send()
    enc_cp().wait_send()
    finish1()
    finish2()


SQUARE = (
    "w_enc_src",
    "w_mesh_self",
    "w_mesh_agg",
    "w_proc_send",
    "w_proc_recv",
    "w_proc_self",
    "w_proc_agg",
    "w_dec_send",
    "w_dec_recv",
    "w_grid_self",
    "w_grid_agg",
)
WEIGHTS = ("w_grid_in",) + SQUARE + ("mesh_emb", "w_grid_out")


def shards(
    grid_in,
    mesh_emb,
    enc_dest,
    enc_node,
    enc_dist,
    dec_dist,
    mesh_src,
    proc_dist,
    w_grid_in,
    w_enc_src,
    w_enc_dist,
    w_mesh_self,
    w_mesh_agg,
    w_proc_send,
    w_proc_recv,
    w_proc_dist,
    w_proc_self,
    w_proc_agg,
    w_dec_send,
    w_dec_recv,
    w_dec_dist,
    w_grid_self,
    w_grid_agg,
    w_grid_out,
):
    n_lat, n_lon = lax.axis_size("lat"), lax.axis_size("lon")
    cells, variables = grid_in.shape
    m, width = mesh_emb.shape
    degree = mesh_src.shape[1]
    local = locals()
    hbm = [local[name] for name in WEIGHTS[:-1]] + [w_grid_out.T]
    vmem = pl.BlockSpec(memory_space=pltpu.VMEM)
    any_space = pl.BlockSpec(memory_space=pl.ANY)
    out = pl.pallas_call(
        functools.partial(kernel, n_lat, n_lon, WEIGHTS),
        out_shape=jax.ShapeDtypeStruct((variables, cells), BF16),
        in_specs=[vmem] * 10 + [any_space] * len(WEIGHTS),
        out_specs=vmem,
        scratch_shapes=[
            pltpu.VMEM((m, width), BF16),
            pltpu.VMEM((len(SQUARE), width, width), BF16),
            pltpu.VMEM((variables, width), BF16),
            pltpu.VMEM((variables, width), BF16),
            pltpu.VMEM((8, cells), F32),
            pltpu.VMEM((8, cells), I32),
            pltpu.VMEM((cells, 8), F32),
            pltpu.VMEM((cells, 128), I32),
            pltpu.VMEM((cells, 128), I32),
            pltpu.VMEM((degree * m, 128), I32),
            pltpu.VMEM((m, degree), F32),
            pltpu.VMEM((cells, width), BF16),
            pltpu.VMEM((2, cells, width), BF16),
            pltpu.VMEM((8, m, width), BF16),
            pltpu.VMEM((8, m, width), BF16),
            pltpu.VMEM((2, m, width), BF16),
            pltpu.VMEM((m, width), F32),
            pltpu.VMEM((m, width), F32),
            pltpu.VMEM((m, width), BF16),
            pltpu.VMEM((UNITS, m, width), BF16),
            pltpu.VMEM((UNITS, m, width), BF16),
            pltpu.VMEM((degree * m, width), F32),
            pltpu.VMEM((cells, width), F32),
            pltpu.VMEM((cells, width), F32),
            pltpu.VMEM((cells, width), F32),
            pltpu.SemaphoreType.DMA((len(WEIGHTS),)),
            pltpu.SemaphoreType.DMA((ENC_SEMS,)),
            pltpu.SemaphoreType.DMA((ENC_SEMS,)),
            pltpu.SemaphoreType.DMA((HALO_SEMS,)),
            pltpu.SemaphoreType.DMA((HALO_SEMS,)),
            pltpu.SemaphoreType.DMA((HALO_SEMS,)),
            pltpu.SemaphoreType.DMA((HALO_SEMS,)),
        ],
        compiler_params=pltpu.CompilerParams(
            collective_id=0, has_side_effects=True, vmem_limit_bytes=67_000_000
        ),
    )(
        grid_in.T,
        enc_dest.T,
        enc_node.T,
        enc_dist.T,
        dec_dist.T,
        mesh_src.T,
        proc_dist.T,
        w_enc_dist.reshape(1, width),
        w_proc_dist.reshape(1, width),
        w_dec_dist.reshape(1, width),
        *hbm,
    )
    return out.T


def solution(mesh):
    split = P(("lat", "lon"), None)
    in_specs = (split,) * 8 + (P(),) * 16
    return jax.shard_map(shards, mesh=mesh, in_specs=in_specs, out_specs=split, check_vma=False)
```

```python
import functools

import jax
import jax.numpy as jnp
from jax import lax
from jax.experimental import pallas as pl
from jax.experimental.pallas import tpu as pltpu
from jax.sharding import PartitionSpec as P

BF16 = jnp.bfloat16
F32 = jnp.float32
I32 = jnp.int32
QUARTERS = 4
LAST = QUARTERS - 1

PARTNER, CROSS, LEFT, RIGHT = range(4)

XL, XR, PL_, PR, OL, OR, XC, PC = range(8)

U_OWN, U_PART, U_CROSS = 0, 1, 3
U_SIDE = {"own": (2, 5), "part": (4, 7), "cross": (6, 8)}
UNITS = 9

ENC_SEMS = 5 * QUARTERS + 3
HALO_SEMS = 8 * QUARTERS


def silu_of_half(h):
    return h + h * jnp.tanh(h)


def silu(v):
    return silu_of_half(0.5 * v)


def mm(a, b):
    return jnp.dot(a, b, preferred_element_type=F32)


def one_hot(keys, base, width):
    lane = lax.broadcasted_iota(I32, keys.shape, 1)
    shifted = keys - base
    pieces = [
        jnp.where(shifted == lane + g * 128, 1.0, 0.0).astype(BF16) for g in range(width // 128)
    ]
    return jnp.concatenate(pieces, axis=1)


def kernel(
    n_lat,
    n_lon,
    weights,
    grid_t,
    dest,
    node,
    enc_d,
    dec_d,
    src,
    proc_d,
    w_enc_dist,
    w_proc_dist,
    w_dec_dist,
    *refs,
):
    hbm = dict(zip(weights, refs[: len(weights)]))
    (
        out,
        emb,
        wv_all,
        w_in,
        w_out,
        cell_keys,
        cell_rows,
        cell_cols,
        key1_lanes,
        key0_lanes,
        proc_lanes,
        proc_cols,
        grid_h,
        msg,
        sb,
        rb,
        ss,
        own_c,
        pre,
        mesh_h,
        table1,
        table2,
        acc,
        near_buf,
        far_buf,
        u_buf,
        w_sems,
        enc_send,
        enc_recv,
        h1_send,
        h1_recv,
        h2_send,
        h2_recv,
    ) = refs[len(weights) :]
    m, width = emb.shape
    cells = grid_t.shape[1]
    degree = src.shape[0]
    quarter = m // QUARTERS
    half = m // 2
    block = min(256, cells)
    wide = min(512, cells)

    lat = lax.axis_index("lat")
    lon = lax.axis_index("lon")
    core = lat % 2
    toward = 1 - 2 * core
    partner = (lat + toward, lon)
    cross = ((lat - toward + n_lat) % n_lat, lon)
    left = (lat, (lon - 1 + n_lon) % n_lon)
    right = (lat, (lon + 1) % n_lon)
    peers = (partner, cross, left, right)

    square = [name for name in weights if name in SQUARE]
    w_at = {name: wv_all.at[i] for i, name in enumerate(square)}
    w_at["w_grid_in"] = w_in
    w_at["mesh_emb"] = emb
    w_at["w_grid_out"] = w_out
    fetches = {
        name: pltpu.make_async_copy(hbm[name], w_at[name], w_sems.at[i])
        for i, name in enumerate(weights)
    }
    for name in weights:
        fetches[name].start()
    barrier = pltpu.get_barrier_semaphore()
    for peer in peers:
        pl.semaphore_signal(
            barrier, inc=1, device_id=peer, device_id_type=pl.DeviceIdType.MESH
        )

    def weight(name):
        return w_at[name][...]

    def remote(src_ref, dst_ref, send, recv, i, peer):
        return pltpu.make_async_remote_copy(
            src_ref=src_ref,
            dst_ref=dst_ref,
            send_sem=send.at[i],
            recv_sem=recv.at[i],
            device_id=peers[peer],
            device_id_type=pl.DeviceIdType.MESH,
        )

    shift = m.bit_length() - 1
    lon_shift = n_lon.bit_length() - 1

    def places(patch):
        d_row = (patch >> lon_shift) - lat
        side = ((patch & (n_lon - 1)) - lon + 1) & (n_lon - 1)
        return d_row == 0, d_row == toward, side

    def gather_key(patch, at):
        own, part, side = places(patch)
        upper = (at >= half).astype(I32)
        centre = jnp.where(own, U_OWN, jnp.where(part, U_PART, U_CROSS)) * m + at
        first = jnp.where(own, U_SIDE["own"][0], jnp.where(part, U_SIDE["part"][0], U_SIDE["cross"][0]))
        second = jnp.where(own, U_SIDE["own"][1], jnp.where(part, U_SIDE["part"][1], U_SIDE["cross"][1]))
        unit = jnp.where(upper == 1, second, first)
        beside = unit * m + jnp.where(side == 2, half, 0) + at - upper * half
        return jnp.where(side == 1, centre, beside)

    patch1 = dest[1:2, :]
    node1 = node[1:2, :]
    own1, part1, side1 = places(patch1)
    slot_l = jnp.where(own1, OL, jnp.where(part1, PL_, XL))
    slot_r = jnp.where(own1, OR, jnp.where(part1, PR, XR))
    slot_c = jnp.where(part1, PC, XC)
    slot = jnp.where(side1 == 0, slot_l, jnp.where(side1 == 2, slot_r, slot_c))
    cell_rows[0:1, :] = slot * m + node1
    cell_rows[1:2, :] = node[0:1, :]
    cell_keys[...] = jnp.zeros_like(cell_keys)
    cell_keys[0:1, :] = node[0:1, :].astype(F32)
    cell_keys[1:2, :] = gather_key(patch1, node1).astype(F32)
    cell_keys[2:4, :] = enc_d[...]
    cell_keys[4:6, :] = dec_d[...]
    cell_cols[...] = jnp.transpose(cell_keys[...])

    fetches["w_grid_in"].wait()
    fetches["w_enc_src"].wait()
    w_in[...] = w_in[...] * 0.5
    w_at["w_enc_src"][...] = weight("w_enc_src") * 0.5
    half_dist = 0.5 * w_enc_dist[...]

    def embed(b, carry):
        rows = pl.ds(pl.multiple_of(b * block, block), block)
        part = grid_t[:, rows]
        h = silu_of_half(
            lax.dot_general(part, w_in[...], (((0,), (0,)), ((), ())), preferred_element_type=F32)
        ).astype(BF16)
        grid_h[rows, :] = h
        e = mm(h, weight("w_enc_src"))
        cols = cell_cols[rows, :]
        for k in range(2):
            msg[k, rows, :] = silu_of_half(e + cols[:, 2 + k : 3 + k] * half_dist).astype(BF16)
        return carry

    lax.fori_loop(0, cells // block, embed, 0)
    pl.semaphore_wait(barrier, 4)

    def enc_x(side, q):
        rows = pl.ds(q * quarter, quarter)
        return remote(
            sb.at[side, rows], rb.at[side, rows], enc_send, enc_recv, 2 * q + side, CROSS
        )

    def enc_p(side):
        return remote(
            sb.at[2 + side], rb.at[2 + side], enc_send, enc_recv, 2 * QUARTERS + side, PARTNER
        )

    def enc_side(side, q):
        rows = pl.ds(q * quarter, quarter)
        return remote(
            ss.at[side, rows],
            rb.at[4 + side, rows],
            enc_send,
            enc_recv,
            2 * QUARTERS + 2 + 2 * q + side,
            LEFT if side == 0 else RIGHT,
        )

    def enc_cx(q):
        rows = pl.ds(q * quarter, quarter)
        return remote(
            sb.at[XC, rows], rb.at[XC, rows], enc_send, enc_recv, 4 * QUARTERS + 2 + q, CROSS
        )

    def enc_cp():
        return remote(sb.at[PC], rb.at[PC], enc_send, enc_recv, 5 * QUARTERS + 2, PARTNER)

    def relay_sums(q):
        rows = pl.ds(q * quarter, quarter)
        for side in range(2):
            enc_x(side, q).wait_recv()
            if q == 0:
                enc_p(side).wait_recv()
            total = (
                sb[4 + side, rows, :].astype(F32)
                + rb[side, rows, :].astype(F32)
                + rb[2 + side, rows, :].astype(F32)
            )
            ss[side, rows, :] = total.astype(BF16)
        for side in range(2):
            enc_side(side, q).start()

    def scatter(row, base, which, rows):
        keys = cell_rows[row : row + 1, :] - base
        sel = jnp.where(lax.broadcasted_iota(I32, (rows, cells), 0) == keys, 1.0, 0.0).astype(BF16)
        return mm(sel, msg[which])

    def cell_block(b):
        return pl.ds(b * wide, wide)

    def cell_terms(blocks):
        for b in blocks:
            rows = cell_block(b)
            h = grid_h[rows, :]
            recv = mm(h, weight("w_dec_recv"))
            cols = cell_cols[rows, :]
            near_buf[rows, :] = recv + cols[:, 4:5] * w_dec_dist[...]
            far_buf[rows, :] = recv + cols[:, 5:6] * w_dec_dist[...]
            u_buf[rows, :] = mm(h, weight("w_grid_self"))
            key0_lanes[rows, :] = jnp.broadcast_to(cols[:, 0:1], (wide, 128)).astype(I32)
            key1_lanes[rows, :] = jnp.broadcast_to(cols[:, 1:2], (wide, 128)).astype(I32)

    def mesh_keys():
        mesh_key = gather_key(src[...] >> shift, src[...] & (m - 1)).astype(F32)
        mesh_key_t = jnp.transpose(mesh_key)
        proc_cols[...] = jnp.transpose(proc_d[...])
        for j in range(degree):
            lanes = jnp.broadcast_to(mesh_key_t[:, j : j + 1], (m, 128)).astype(I32)
            for q in range(QUARTERS):
                proc_lanes[pl.ds((q * degree + j) * quarter, quarter), :] = lanes[
                    q * quarter : (q + 1) * quarter
                ]

    for upper in range(2):
        for side in range(2):
            part = scatter(0, side * m + upper * half, 1, half)
            sb[side, pl.ds(upper * half, half), :] = part.astype(BF16)
        for q in range(2 * upper, 2 * upper + 2):
            for side in range(2):
                enc_x(side, q).start()

    def partial_step(s, carry):
        sb[s] = scatter(0, s * m, 1, m).astype(BF16)

        @pl.when(s == PR)
        def _():
            for side in range(2):
                enc_p(side).start()

        @pl.when(s == OR)
        def _():
            relay_sums(0)

        @pl.when(s == XC)
        def _():
            for q in range(QUARTERS):
                enc_cx(q).start()

        @pl.when(s == PC)
        def _():
            enc_cp().start()

        return carry

    lax.fori_loop(2, 8, partial_step, 0)
    relay_sums(1)
    mesh_keys()
    own_c[...] = scatter(1, 0, 0, m)
    fetches["w_dec_recv"].wait()
    fetches["w_grid_self"].wait()
    blocks = cells // wide
    cell_terms(range(0, blocks // 2))
    relay_sums(2)
    cell_terms(range(blocks // 2, blocks))
    for name in (
        "mesh_emb",
        "w_mesh_self",
        "w_mesh_agg",
        "w_proc_send",
        "w_proc_recv",
        "w_proc_self",
    ):
        fetches[name].wait()
    pre[...] = mm(emb[...], weight("w_mesh_self"))
    relay_sums(3)

    enc_cp().wait_recv()

    def halo(table, send, recv):
        def own(q, peer):
            src_ref = table.at[U_OWN, pl.ds(q * quarter, quarter)]
            if peer == PARTNER:
                dst = table.at[U_PART, pl.ds(q * quarter, quarter)]
            elif peer == CROSS:
                dst = table.at[U_CROSS, pl.ds(q * quarter, quarter)]
            else:
                dst = side_rows("own", 1 if peer == LEFT else 0, q)
            return remote(src_ref, dst, send, recv, 4 * q + peer, peer)

        def side_rows(owner, side, q):
            unit = U_SIDE[owner][q // 2]
            return table.at[unit, pl.ds(side * half + (q % 2) * quarter, quarter)]

        def forward(side, q, peer):
            dst = side_rows("part" if peer == PARTNER else "cross", side, q)
            index = 4 * QUARTERS + 4 * q + 2 * side + peer
            if peer == CROSS and q == LAST:
                src_ref = table.at[U_CROSS, pl.ds(q * quarter, quarter)]
                return remote(src_ref, dst, send, recv, index, RIGHT if side == 0 else LEFT)
            return remote(side_rows("own", side, q), dst, send, recv, index, peer)

        def start_own(q):
            for peer in (LEFT, RIGHT, CROSS, PARTNER):
                own(q, peer).start()

        def pass_on(q):
            own(q, RIGHT).wait_recv()
            own(q, LEFT).wait_recv()
            for side in range(2):
                if q != LAST:
                    forward(side, q, CROSS).start()
                forward(side, q, PARTNER).start()

        def turn_corner():
            own(LAST, CROSS).wait_recv()
            for side in range(2):
                forward(side, LAST, CROSS).start()

        def wait_forwarded(peer, quarters):
            for q in quarters:
                for side in range(2):
                    forward(side, q, peer).wait_recv()

        def before(u):
            @pl.when(u == 3)
            def _():
                pass_on(2)
                for q in range(QUARTERS):
                    if q != LAST:
                        own(q, CROSS).wait_recv()

            @pl.when(u == 4)
            def _():
                wait_forwarded(PARTNER, (0, 1))

            @pl.when(u == 5)
            def _():
                pass_on(LAST)

            @pl.when(u == 6)
            def _():
                wait_forwarded(CROSS, (0, 1))

            @pl.when(u == 7)
            def _():
                wait_forwarded(PARTNER, (2, 3))

        def before_partner():
            for q in range(QUARTERS):
                own(q, PARTNER).wait_recv()

        def before_last(units):
            if 6 in units:
                wait_forwarded(CROSS, (0, 1))
            if 7 in units:
                wait_forwarded(PARTNER, (2, 3))
            wait_forwarded(CROSS, (2, 3))

        def finish():
            for q in range(QUARTERS):
                for peer in range(4):
                    own(q, peer).wait_send()
                for side in range(2):
                    for peer in (PARTNER, CROSS):
                        forward(side, q, peer).wait_send()

        return start_own, before_partner, pass_on, turn_corner, before, before_last, finish

    start1, partner1, pass1, turn1, before1, last1, finish1 = halo(table1, h1_send, h1_recv)
    start2, partner2, pass2, turn2, before2, last2, finish2 = halo(table2, h2_send, h2_recv)

    for q in range(QUARTERS):
        rows = pl.ds(q * quarter, quarter)
        for side in range(2):
            enc_side(side, q).wait_recv()
        enc_cx(q).wait_recv()
        total = own_c[rows, :]
        for i in range(4, 8):
            total = total + rb[i, rows, :].astype(F32)
        upd = pre[rows, :] + mm(total.astype(BF16), weight("w_mesh_agg"))
        h = (emb[rows, :].astype(F32) + silu(upd)).astype(BF16)
        mesh_h[rows, :] = h
        table1[U_OWN, rows, :] = mm(h, weight("w_proc_send")).astype(BF16)
        start1(q)
        pre[rows, :] = mm(h, weight("w_proc_recv"))
        own_c[rows, :] = mm(h, weight("w_proc_self"))

    for name in ("w_proc_agg", "w_dec_send"):
        fetches[name].wait()
    group = 2 * QUARTERS
    edge_rows = degree * m // group
    per_group = edge_rows // quarter

    def edges(g):
        return pl.ds(g * edge_rows, edge_rows)

    def units(table, first, last):
        return table[first:last].reshape((last - first) * m, width)

    partner1()
    for g in range(group):
        if g == group // 2:
            pass1(0)
            pass1(1)
        parts = []
        for e in range(g * per_group, (g + 1) * per_group):
            rows = pl.ds(e // degree * quarter, quarter)
            j = e % degree
            parts.append(pre[rows, :] + proc_cols[rows, j : j + 1] * w_proc_dist[...])
        base = jnp.concatenate(parts, axis=0)
        acc[edges(g), :] = base + mm(
            one_hot(proc_lanes[edges(g), :], 0, 2 * m), units(table1, 0, 2)
        )
    turn1()

    def proc_unit(u, carry):
        before1(u)
        for g in range(group):
            acc[edges(g), :] += mm(one_hot(proc_lanes[edges(g), :], u * m, m), table1[u])
        return carry

    lax.fori_loop(2, 6, proc_unit, 0)
    last1((6, 7, 8))
    for q in range(QUARTERS):
        rows = pl.ds(q * quarter, quarter)
        agg = None
        for g in range(q * degree // per_group, (q + 1) * degree // per_group):
            full = acc[edges(g), :] + mm(
                one_hot(proc_lanes[edges(g), :], 6 * m, 3 * m), units(table1, 6, 9)
            )
            messages = silu(full)
            for i in range(per_group):
                one = messages[i * quarter : (i + 1) * quarter]
                agg = one if agg is None else agg + one
        upd = own_c[rows, :] + mm(agg.astype(BF16), weight("w_proc_agg"))
        h = (mesh_h[rows, :].astype(F32) + silu(upd)).astype(BF16)
        table2[U_OWN, rows, :] = mm(h, weight("w_dec_send")).astype(BF16)
        start2(q)

    for b in range(cells // wide):
        rows = cell_block(b)
        near = near_buf[rows, :] + mm(one_hot(key0_lanes[rows, :], 0, m), table2[U_OWN])
        near_buf[rows, :] = silu(near)
    partner2()
    pass2(0)
    turn2()
    pass2(1)
    for b in range(cells // wide):
        rows = cell_block(b)
        far_buf[rows, :] += mm(one_hot(key1_lanes[rows, :], m, m), table2[U_PART])

    def dec_unit(u, carry):
        before2(u)
        for b in range(cells // wide):
            rows = cell_block(b)
            far_buf[rows, :] += mm(one_hot(key1_lanes[rows, :], u * m, m), table2[u])
        return carry

    lax.fori_loop(2, 8, dec_unit, 0)
    last2((8,))
    fetches["w_grid_agg"].wait()
    fetches["w_grid_out"].wait()
    for b in range(cells // wide):
        rows = cell_block(b)
        far = far_buf[rows, :] + mm(
            one_hot(key1_lanes[rows, :], 8 * m, m), table2[8]
        )
        agg = (near_buf[rows, :] + silu(far)).astype(BF16)
        z = silu(u_buf[rows, :] + mm(agg, weight("w_grid_agg"))).astype(BF16)
        change = lax.dot_general(
            w_out[...], z, (((1,), (1,)), ((), ())), preferred_element_type=F32
        )
        out[:, rows] = (grid_t[:, rows].astype(F32) + change).astype(BF16)

    for side in range(2):
        for q in range(QUARTERS):
            enc_x(side, q).wait_send()
            enc_side(side, q).wait_send()
        enc_p(side).wait_send()
    for q in range(QUARTERS):
        enc_cx(q).wait_send()
    enc_cp().wait_send()
    finish1()
    finish2()


SQUARE = (
    "w_enc_src",
    "w_mesh_self",
    "w_mesh_agg",
    "w_proc_send",
    "w_proc_recv",
    "w_proc_self",
    "w_proc_agg",
    "w_dec_send",
    "w_dec_recv",
    "w_grid_self",
    "w_grid_agg",
)
WEIGHTS = ("w_grid_in",) + SQUARE + ("mesh_emb", "w_grid_out")


def shards(
    grid_in,
    mesh_emb,
    enc_dest,
    enc_node,
    enc_dist,
    dec_dist,
    mesh_src,
    proc_dist,
    w_grid_in,
    w_enc_src,
    w_enc_dist,
    w_mesh_self,
    w_mesh_agg,
    w_proc_send,
    w_proc_recv,
    w_proc_dist,
    w_proc_self,
    w_proc_agg,
    w_dec_send,
    w_dec_recv,
    w_dec_dist,
    w_grid_self,
    w_grid_agg,
    w_grid_out,
):
    n_lat, n_lon = lax.axis_size("lat"), lax.axis_size("lon")
    cells, variables = grid_in.shape
    m, width = mesh_emb.shape
    degree = mesh_src.shape[1]
    local = locals()
    hbm = [local[name] for name in WEIGHTS[:-1]] + [w_grid_out.T]
    vmem = pl.BlockSpec(memory_space=pltpu.VMEM)
    any_space = pl.BlockSpec(memory_space=pl.ANY)
    out = pl.pallas_call(
        functools.partial(kernel, n_lat, n_lon, WEIGHTS),
        out_shape=jax.ShapeDtypeStruct((variables, cells), BF16),
        in_specs=[vmem] * 10 + [any_space] * len(WEIGHTS),
        out_specs=vmem,
        scratch_shapes=[
            pltpu.VMEM((m, width), BF16),
            pltpu.VMEM((len(SQUARE), width, width), BF16),
            pltpu.VMEM((variables, width), BF16),
            pltpu.VMEM((variables, width), BF16),
            pltpu.VMEM((8, cells), F32),
            pltpu.VMEM((8, cells), I32),
            pltpu.VMEM((cells, 8), F32),
            pltpu.VMEM((cells, 128), I32),
            pltpu.VMEM((cells, 128), I32),
            pltpu.VMEM((degree * m, 128), I32),
            pltpu.VMEM((m, degree), F32),
            pltpu.VMEM((cells, width), BF16),
            pltpu.VMEM((2, cells, width), BF16),
            pltpu.VMEM((8, m, width), BF16),
            pltpu.VMEM((8, m, width), BF16),
            pltpu.VMEM((2, m, width), BF16),
            pltpu.VMEM((m, width), F32),
            pltpu.VMEM((m, width), F32),
            pltpu.VMEM((m, width), BF16),
            pltpu.VMEM((UNITS, m, width), BF16),
            pltpu.VMEM((UNITS, m, width), BF16),
            pltpu.VMEM((degree * m, width), F32),
            pltpu.VMEM((cells, width), F32),
            pltpu.VMEM((cells, width), F32),
            pltpu.VMEM((cells, width), F32),
            pltpu.SemaphoreType.DMA((len(WEIGHTS),)),
            pltpu.SemaphoreType.DMA((ENC_SEMS,)),
            pltpu.SemaphoreType.DMA((ENC_SEMS,)),
            pltpu.SemaphoreType.DMA((HALO_SEMS,)),
            pltpu.SemaphoreType.DMA((HALO_SEMS,)),
            pltpu.SemaphoreType.DMA((HALO_SEMS,)),
            pltpu.SemaphoreType.DMA((HALO_SEMS,)),
        ],
        compiler_params=pltpu.CompilerParams(
            collective_id=0, has_side_effects=True, vmem_limit_bytes=67_000_000
        ),
    )(
        grid_in.T,
        enc_dest.T,
        enc_node.T,
        enc_dist.T,
        dec_dist.T,
        mesh_src.T,
        proc_dist.T,
        w_enc_dist.reshape(1, width),
        w_proc_dist.reshape(1, width),
        w_dec_dist.reshape(1, width),
        *hbm,
    )
    return out.T


def solution(mesh):
    split = P(("lat", "lon"), None)
    in_specs = (split,) * 8 + (P(),) * 16
    return jax.shard_map(shards, mesh=mesh, in_specs=in_specs, out_specs=split, check_vma=False)
```
